32 devices in a mesh: ty: 8 (over y, x, core), tx: 4 (over z).
Axes of the slice: x: 2, y: 2, z: 4, core: 2. Of those that a mesh axis runs over, the one named last changes fastest.
Arguments:
- queries: bfloat16 [64, 64, 1024], P('ty', 'tx'), may hold values from -6 to 6
- fine_key_rows: bfloat16 [64, 64, 1024], P('ty', 'tx'), may hold values from -6 to 6
- fine_value_rows: bfloat16 [64, 64, 1024], P('ty', 'tx'), may hold values from -6 to 6
- fine_query_tangent: bfloat16 [64, 64, 1024], P('ty', 'tx'), may hold values from -6 to 6
- fine_key_tangent: bfloat16 [64, 64, 1024], P('ty', 'tx'), may hold values from -6 to 6
- fine_value_tangent: bfloat16 [64, 64, 1024], P('ty', 'tx'), may hold values from -6 to 6
- fine_head_scale: float32 [16], replicated, may hold values from 2 to 20
- merged_token_weight: bfloat16 [1024, 1024], replicated, may hold values from -0.1875 to 0.1875
- time_plan_index: int32 [2], replicated, may hold values from 0 to 999
- time_modulation_weight: float32 [256, 4096], replicated, may hold values from -0.09375 to 0.09375
- coarse_projection_weight: bfloat16 [1024, 16, 192], P(None, 'tx'), may hold values from -0.1875 to 0.1875
- coarse_head_scale: float32 [16], P('tx'), may hold values from 2 to 20
- head_output_weight: bfloat16 [16, 64, 1024], P('tx'), may hold values from -0.1875 to 0.1875
- up_projection_weight: bfloat16 [1024, 4096], P(None, 'tx'), may hold values from -0.1875 to 0.1875
- down_projection_weight: bfloat16 [4096, 1024], P('tx'), may hold values from -0.09375 to 0.09375
Outputs:
- fine_out: bfloat16 [64, 64, 1024], P('ty', 'tx')
- fine_tangent: bfloat16 [64, 64, 1024], P('ty', 'tx')
- coarse_out: bfloat16 [16, 16, 1024], P('ty', 'tx')
- coarse_tangent: bfloat16 [16, 16, 1024], P('ty', 'tx')
The draws below stay inside these ranges and needn't reach their ends.
Inputs may be any that keep to these rules, and one draw needn't show every extreme that they name: `time_plan_index`: two indices into the plan t_k = k / 1000; the larger gives t, the smaller r.
All inputs are finite; a program needn't handle non-finite values.
Results may differ from the reference program's by a relative error of at most 0.035.
Values may be sent and summed in bfloat16 or wider, within the bound.
No kernel may reach another device: no remote copies, remote signals or barrier semaphores. Data moves between devices by JAX's collectives and lax.ppermute only.
A program may use at most 64 MiB of HBM per device.

```python
import math
import jax
import jax.numpy as jnp
from jax import lax

D = 1024
HEAD_TOTAL = 16
FF = 4096
EMBED = 128
RADIUS = 3
MERGE = 4
STEPS = 1000
HEAD_SIZE = 64
GRID_R = 64
GRID_C = 64
COARSE_R = 16
COARSE_C = 16


def shard_levels(key, dims, pieces, smallest, high):
    loudness = 1.0
    for axis_at, shards_of in pieces:
        steps = jax.random.uniform(jax.random.fold_in(jax.random.fold_in(key, 6), axis_at), (shards_of,), jnp.float32, smallest / len(pieces), high / len(pieces))
        loudness = loudness * jnp.repeat(jnp.exp(steps), dims[axis_at] // shards_of).reshape((-1,) + (1,) * (len(dims) - 1 - axis_at))
    return loudness


def gaussian(stream_key, extent, width, limit, cuts=(), dtype=jnp.bfloat16):
    drawn = width * jax.random.normal(stream_key, extent, jnp.float32)
    if cuts:
        drawn = drawn * shard_levels(stream_key, extent, cuts, -0.22, 0.18)
    return jnp.clip(drawn, -limit, limit).astype(dtype)


def setup_inputs(seed: int = 0) -> dict:
    splits = jax.random.split(jax.random.key(seed), 16)
    queries = gaussian(splits[0], (GRID_R, GRID_C, D), 1.0, 6.0, ((0, 8), (1, 4)))
    fine_key_rows = gaussian(splits[1], (GRID_R, GRID_C, D), 1.0, 6.0, ((0, 8), (1, 4)))
    fine_value_rows = gaussian(splits[2], (GRID_R, GRID_C, D), 1.0, 6.0, ((0, 8), (1, 4)))
    fine_query_tangent = gaussian(splits[3], (GRID_R, GRID_C, D), 1.0, 6.0, ((0, 8), (1, 4)))
    fine_key_tangent = gaussian(splits[4], (GRID_R, GRID_C, D), 1.0, 6.0, ((0, 8), (1, 4)))
    fine_value_tangent = gaussian(splits[5], (GRID_R, GRID_C, D), 1.0, 6.0, ((0, 8), (1, 4)))
    fine_head_scale = jnp.clip(jnp.exp(jax.random.uniform(splits[6], (HEAD_TOTAL,), jnp.float32, math.log(2.0), math.log(20.0))), 2.0, 20.0)
    merged_token_weight = gaussian(splits[7], (D, D), D ** -0.5, 0.1875)
    time_plan_index = jax.random.randint(splits[8], (2,), 0, STEPS).astype(jnp.int32)
    time_modulation_weight = gaussian(splits[9], (2 * EMBED, 4 * D), (32 * EMBED) ** -0.5, 0.09375, (), jnp.float32)
    coarse_projection_weight = gaussian(splits[10], (D, HEAD_TOTAL, 3 * HEAD_SIZE), D ** -0.5, 0.1875, ((1, 4),))
    coarse_head_scale = jnp.clip(jnp.exp(math.log(20.0) - 2.3025851 * jax.random.uniform(splits[11], (HEAD_TOTAL,), jnp.float32) ** shard_levels(splits[11], (HEAD_TOTAL,), ((0, 4),), -0.2, 0.2)), 2.0, 20.0)
    head_output_weight = gaussian(splits[12], (HEAD_TOTAL, HEAD_SIZE, D), D ** -0.5, 0.1875, ((0, 4),))
    up_projection_weight = gaussian(splits[13], (D, FF), D ** -0.5, 0.1875, ((1, 4),))
    down_projection_weight = gaussian(splits[14], (FF, D), FF ** -0.5, 0.09375, ((0, 4),))
    return dict(queries=queries, fine_key_rows=fine_key_rows, fine_value_rows=fine_value_rows, fine_query_tangent=fine_query_tangent, fine_key_tangent=fine_key_tangent, fine_value_tangent=fine_value_tangent, fine_head_scale=fine_head_scale, merged_token_weight=merged_token_weight, time_plan_index=time_plan_index, time_modulation_weight=time_modulation_weight, coarse_projection_weight=coarse_projection_weight, coarse_head_scale=coarse_head_scale, head_output_weight=head_output_weight, up_projection_weight=up_projection_weight, down_projection_weight=down_projection_weight)


EPSILON = 1e-06

def normed_pair(values, tangent):
    factor = lax.rsqrt(lax.optimization_barrier(jnp.mean(values * values, axis=-1, keepdims=True)) + EPSILON)
    normed = values * factor
    drift = (tangent - normed * lax.optimization_barrier(jnp.mean(normed * tangent, axis=-1, keepdims=True))) * factor
    return (normed, drift)

def modulation(time_plan_index, time_modulation_weight):
    latest = jnp.max(time_plan_index)
    earlier = jnp.min(time_plan_index)
    moment = latest.astype(jnp.float32) / STEPS
    spacing = (latest - earlier).astype(jnp.float32) / STEPS
    halves = EMBED // 2
    angular = 16.0 ** (jnp.arange(halves).astype(jnp.float32) / halves)
    embedded = jnp.concatenate([jnp.cos(angular * moment), jnp.sin(angular * moment), jnp.cos(angular * spacing), jnp.sin(angular * spacing)])
    slopes = jnp.concatenate([-angular * jnp.sin(angular * moment), angular * jnp.cos(angular * moment), -angular * jnp.sin(angular * spacing), angular * jnp.cos(angular * spacing)])
    result = jnp.dot(jnp.stack([embedded, slopes]), time_modulation_weight, precision=lax.Precision.HIGHEST)
    return (jnp.split(result[0], 4), jnp.split(result[1], 4))

def conditioned(values, tangent, offset, stretch, offset_drift, stretch_drift):
    normed, drift = normed_pair(values, tangent)
    primal = (normed * (1.0 + stretch) + offset).astype(jnp.bfloat16)
    moving = (drift * (1.0 + stretch) + normed * stretch_drift + offset_drift).astype(jnp.bfloat16)
    return (primal, moving)

def gelu_tanh(values):
    return jax.nn.gelu(values, approximate=True)

def window(array, step_down, step_across):
    return array[step_down:step_down + GRID_R, step_across:step_across + GRID_C]

def fine_head(head_entries):
    query_normalized, query_velocity, key_normalized, key_velocity, value_head, value_drift, factor = head_entries
    border = ((RADIUS, RADIUS), (RADIUS, RADIUS), (0, 0))
    key_pad = jnp.pad(key_normalized.astype(jnp.float32), border)
    key_drift_pad = jnp.pad(key_velocity.astype(jnp.float32), border)
    value_pad = jnp.pad(value_head.astype(jnp.float32), border)
    value_drift_pad = jnp.pad(value_drift.astype(jnp.float32), border)
    inside = jnp.pad(jnp.ones((GRID_R, GRID_C), jnp.float32), RADIUS)
    query_float = query_normalized.astype(jnp.float32)
    query_drift_float = query_velocity.astype(jnp.float32)
    weight_sum = jnp.zeros((GRID_R, GRID_C), jnp.float32)
    slope_sum = jnp.zeros((GRID_R, GRID_C), jnp.float32)
    value_sum = jnp.zeros(query_float.shape, jnp.float32)
    turned = jnp.zeros(query_float.shape, jnp.float32)
    shifted = jnp.zeros(query_float.shape, jnp.float32)
    for step_down in range(2 * RADIUS + 1):
        for step_across in range(2 * RADIUS + 1):
            keys_here = window(key_pad, step_down, step_across)
            scores = factor * lax.optimization_barrier(jnp.sum(query_float * keys_here, axis=-1))
            slopes = factor * (lax.optimization_barrier(jnp.sum(query_drift_float * keys_here, axis=-1)) + lax.optimization_barrier(jnp.sum(query_float * window(key_drift_pad, step_down, step_across), axis=-1)))
            weights = jnp.exp(scores) * window(inside, step_down, step_across)
            tilted = weights * slopes
            weights_low = weights.astype(jnp.bfloat16).astype(jnp.float32)
            tilted_low = tilted.astype(jnp.bfloat16).astype(jnp.float32)
            values_here = window(value_pad, step_down, step_across)
            weight_sum = weight_sum + weights
            slope_sum = slope_sum + tilted
            value_sum = value_sum + weights_low[..., None] * values_here
            turned = turned + tilted_low[..., None] * values_here
            shifted = shifted + weights_low[..., None] * window(value_drift_pad, step_down, step_across)
    inverse = 1.0 / weight_sum[..., None]
    output = value_sum * inverse
    return (output, (turned + shifted) * inverse - output * (slope_sum[..., None] * inverse))

def coarse_head(head_entries):
    query_normalized, query_velocity, key_normalized, key_velocity, value_head, value_drift, factor = head_entries
    scores = factor * jnp.dot(query_normalized, key_normalized.T, preferred_element_type=jnp.float32)
    slopes = factor * (jnp.dot(query_velocity, key_normalized.T, preferred_element_type=jnp.float32) + jnp.dot(query_normalized, key_velocity.T, preferred_element_type=jnp.float32))
    weights = jnp.exp(scores)
    tilted = weights * slopes
    weights_low = weights.astype(jnp.bfloat16)
    tilted_low = tilted.astype(jnp.bfloat16)
    value_sum = jnp.dot(weights_low, value_head, preferred_element_type=jnp.float32)
    turned = jnp.dot(tilted_low, value_head, preferred_element_type=jnp.float32)
    shifted = jnp.dot(weights_low, value_drift, preferred_element_type=jnp.float32)
    inverse = 1.0 / lax.optimization_barrier(jnp.sum(weights, axis=-1))[:, None]
    output = value_sum * inverse
    return (output, (turned + shifted) * inverse - output * (lax.optimization_barrier(jnp.sum(tilted, axis=-1))[:, None] * inverse))

def pooled(tile_grid):
    return lax.optimization_barrier(jnp.mean(tile_grid.astype(jnp.float32).reshape(GRID_R // MERGE, MERGE, GRID_C // MERGE, MERGE, D), axis=(1, 3))).reshape(-1, D).astype(jnp.bfloat16)

def reference(queries, fine_key_rows, fine_value_rows, fine_query_tangent, fine_key_tangent, fine_value_tangent, fine_head_scale, merged_token_weight, time_plan_index, time_modulation_weight, coarse_projection_weight, coarse_head_scale, head_output_weight, up_projection_weight, down_projection_weight):
    by_head = (GRID_R, GRID_C, HEAD_TOTAL, HEAD_SIZE)
    query_normalized, query_velocity = normed_pair(queries.astype(jnp.float32).reshape(by_head), fine_query_tangent.astype(jnp.float32).reshape(by_head))
    key_normalized, key_velocity = normed_pair(fine_key_rows.astype(jnp.float32).reshape(by_head), fine_key_tangent.astype(jnp.float32).reshape(by_head))

    def head_major_layout(array):
        return jnp.moveaxis(array.astype(jnp.bfloat16).reshape(by_head), 2, 0)
    head_entries = (head_major_layout(query_normalized), head_major_layout(query_velocity), head_major_layout(key_normalized), head_major_layout(key_velocity), head_major_layout(fine_value_rows), head_major_layout(fine_value_tangent), fine_head_scale / HEAD_SIZE)
    output, drift = lax.map(fine_head, head_entries)
    fine_out = jnp.moveaxis(output, 0, 2).reshape(GRID_R, GRID_C, D).astype(jnp.bfloat16)
    fine_tangent = jnp.moveaxis(drift, 0, 2).reshape(GRID_R, GRID_C, D).astype(jnp.bfloat16)
    coarse = jnp.dot(pooled(fine_out), merged_token_weight, preferred_element_type=jnp.float32).astype(jnp.bfloat16)
    coarse_drift = jnp.dot(pooled(fine_tangent), merged_token_weight, preferred_element_type=jnp.float32).astype(jnp.bfloat16)
    primal_mod, drift_mod = modulation(time_plan_index, time_modulation_weight)
    offset_a, stretch_a, offset_m, stretch_m = primal_mod
    offset_ad, stretch_ad, offset_md, stretch_md = drift_mod
    normed, normed_drift = conditioned(coarse.astype(jnp.float32), coarse_drift.astype(jnp.float32), offset_a, stretch_a, offset_ad, stretch_ad)
    packed = coarse_projection_weight.reshape(D, HEAD_TOTAL * 3 * HEAD_SIZE)
    projected_rows = jnp.dot(normed, packed, preferred_element_type=jnp.float32).reshape(-1, HEAD_TOTAL, 3 * HEAD_SIZE)
    projected_velocity = jnp.dot(normed_drift, packed, preferred_element_type=jnp.float32).reshape(-1, HEAD_TOTAL, 3 * HEAD_SIZE)
    coarse_query_rows, coarse_query_velocity = normed_pair(projected_rows[..., :HEAD_SIZE], projected_velocity[..., :HEAD_SIZE])
    coarse_key_rows, coarse_key_velocity = normed_pair(projected_rows[..., HEAD_SIZE:2 * HEAD_SIZE], projected_velocity[..., HEAD_SIZE:2 * HEAD_SIZE])

    def head_leading_layout(array):
        return jnp.moveaxis(array.astype(jnp.bfloat16), 1, 0)
    coarse_entries = (head_leading_layout(coarse_query_rows), head_leading_layout(coarse_query_velocity), head_leading_layout(coarse_key_rows), head_leading_layout(coarse_key_velocity), head_leading_layout(projected_rows[..., 2 * HEAD_SIZE:]), head_leading_layout(projected_velocity[..., 2 * HEAD_SIZE:]), coarse_head_scale / HEAD_SIZE)
    attended, attended_drift = lax.map(coarse_head, coarse_entries)
    merged_heads = jnp.moveaxis(attended, 0, 1).reshape(-1, D).astype(jnp.bfloat16)
    merged_drift = jnp.moveaxis(attended_drift, 0, 1).reshape(-1, D).astype(jnp.bfloat16)
    out_packed = head_output_weight.reshape(D, D)
    updated = coarse.astype(jnp.float32) + jnp.dot(merged_heads, out_packed, preferred_element_type=jnp.float32)
    updated_drift = coarse_drift.astype(jnp.float32) + jnp.dot(merged_drift, out_packed, preferred_element_type=jnp.float32)
    mlp_source, mlp_source_drift = conditioned(updated, updated_drift, offset_m, stretch_m, offset_md, stretch_md)
    hidden_in = jnp.dot(mlp_source, up_projection_weight, preferred_element_type=jnp.float32)
    hidden_in_drift = jnp.dot(mlp_source_drift, up_projection_weight, preferred_element_type=jnp.float32)
    hidden_out, hidden_out_drift = jax.jvp(gelu_tanh, (hidden_in,), (hidden_in_drift,))
    grown = jnp.dot(hidden_out.astype(jnp.bfloat16), down_projection_weight, preferred_element_type=jnp.float32)
    grown_drift = jnp.dot(hidden_out_drift.astype(jnp.bfloat16), down_projection_weight, preferred_element_type=jnp.float32)
    coarse_out = (updated + grown).astype(jnp.bfloat16).reshape(COARSE_R, COARSE_C, D)
    coarse_tangent = (updated_drift + grown_drift).astype(jnp.bfloat16).reshape(COARSE_R, COARSE_C, D)
    return (fine_out, fine_tangent, coarse_out, coarse_tangent)
```

```python
import functools
import math

import jax
import jax.numpy as jnp
import numpy as np
from jax import lax
from jax.experimental import pallas as pl
from jax.experimental.pallas import tpu as pltpu
from jax.sharding import PartitionSpec as P

EMBED = 128
RADIUS = 3
MERGE = 4
STEPS = 1000
EPSILON = 1e-06
LANES = 128
LOG2E = math.log2(math.e)
F32 = jnp.float32
BF16 = jnp.bfloat16


def dot(a, b):
    return jnp.dot(a, b, preferred_element_type=F32)


def dot_nt(a, b):
    return lax.dot_general(a, b, (((1,), (1,)), ((), ())), preferred_element_type=F32)


def block_ones(width, head, value):
    row = lax.broadcasted_iota(jnp.int32, (width, width), 0)
    col = lax.broadcasted_iota(jnp.int32, (width, width), 1)
    same = lax.shift_right_logical(row, head) == lax.shift_right_logical(col, head)
    return jnp.where(same, value, 0.0).astype(BF16)


def head_mean(values, ones):
    high = values.astype(BF16)
    low = (values - high.astype(F32)).astype(BF16)
    return dot(high, ones) + dot(low, ones)


def head_pair(values, tangent, ones):
    factor = lax.rsqrt(head_mean(values * values, ones) + EPSILON)
    normed = values * factor
    drift = (tangent - normed * head_mean(normed * tangent, ones)) * factor
    return normed.astype(BF16), drift.astype(BF16)


def row_pair(values, tangent):
    factor = lax.rsqrt(jnp.mean(values * values, axis=-1, keepdims=True) + EPSILON)
    normed = values * factor
    drift = (tangent - normed * jnp.mean(normed * tangent, axis=-1, keepdims=True)) * factor
    return normed, drift


def conditioned(values, tangent, mod, part, width):
    normed, drift = row_pair(values, tangent)
    offset = mod[0:1, 2 * part * width : (2 * part + 1) * width]
    stretch = mod[0:1, (2 * part + 1) * width : (2 * part + 2) * width]
    offset_drift = mod[1:2, 2 * part * width : (2 * part + 1) * width]
    stretch_drift = mod[1:2, (2 * part + 1) * width : (2 * part + 2) * width]
    primal = (normed * (1.0 + stretch) + offset).astype(BF16)
    moving = (drift * (1.0 + stretch) + normed * stretch_drift + offset_drift).astype(BF16)
    return primal, moving


def side(axis, phase):
    at = lax.axis_index(axis)
    after = (at & 1) == phase
    exists = jnp.where(after, at + 1 < lax.axis_size(axis), at > 0)
    return after, exists


def couples(count, phase):
    return [
        edge for i in range(phase, count - 1, 2) for edge in ((i, i + 1), (i + 1, i))
    ]


def partner(count, step, back=False):
    if count & (count - 1) == 0:
        return [(i, i ^ step) for i in range(count)]
    return [(i, (i - step if back else i + step) % count) for i in range(count)]


def gathered(value, axis):
    count = lax.axis_size(axis)
    return [value] + [
        lax.ppermute(value, axis, partner(count, step)) for step in range(1, count)
    ]


def returned(pieces, axis):
    count = lax.axis_size(axis)
    return [
        lax.ppermute(piece, axis, partner(count, step, True))
        for step, piece in zip(range(1, count), pieces)
    ]


def attend(query, query_drift, key, key_drift, value, value_drift, mask, factors, head):
    count = query.shape[0]
    lane = lax.broadcasted_iota(jnp.int32, (1, LANES), 1)
    first = (lane < head).astype(F32).astype(BF16)
    second = (lane >= head).astype(F32).astype(BF16)
    query_0, query_1 = query * first, query * second
    drift_0, drift_1 = query_drift * first, query_drift * second
    score = dot_nt(jnp.concatenate([query_0, query_1], 0), key)
    slope = dot_nt(
        jnp.concatenate(
            [
                jnp.concatenate([drift_0, query_0], 1),
                jnp.concatenate([drift_1, query_1], 1),
            ],
            0,
        ),
        jnp.concatenate([key, key_drift], 1),
    )
    weights, tilted = [], []
    for place, factor in enumerate(factors):
        rows = slice(place * count, (place + 1) * count)
        weight = jnp.exp2(score[rows] * (factor * LOG2E)) * mask
        weights.append(weight)
        tilted.append(weight * (slope[rows] * factor))
    weight = jnp.concatenate(weights, 0).astype(BF16)
    tilt = jnp.concatenate(tilted, 0).astype(BF16)
    ones = jnp.ones((key.shape[0], LANES), BF16)
    mixed = dot(weight, jnp.concatenate([value, value_drift], 1))
    turned = dot(tilt, value)
    total = dot(weight, ones)
    lean = dot(tilt, ones)

    def own(stack):
        return jnp.where(lane < head, stack[:count], stack[count:])

    return own(mixed[:, :LANES]), own(mixed[:, LANES:] + turned), own(total), own(lean)


def near(key_row, key_column, columns, count):
    place = lax.broadcasted_iota(jnp.int32, (count, 1), 0)
    shift = columns.bit_length() - 1
    row = lax.shift_right_logical(place, shift)
    column = place & (columns - 1)
    close = (jnp.abs(row - key_row) <= RADIUS) & (jnp.abs(column - key_column) <= RADIUS)
    return jnp.where(close, 1.0, 0.0)


def pack_kernel(head_tail, key, value, key_drift, value_drift, y0, y1, z0, z1):
    rows, columns, width = key.shape
    strip = RADIUS * columns
    band = head_tail.shape[1]
    for array, ref in enumerate((key, value, key_drift, value_drift)):
        flat = ref[...].reshape(rows * columns, width)
        for phase, (y, z) in enumerate(((y0, z0), (y1, z1))):
            down, _ = side("ty", phase)
            start = jnp.where(down, rows - RADIUS, 0)
            y[array * strip : (array + 1) * strip] = ref[pl.ds(start, RADIUS)].reshape(
                strip, width
            )
            right, _ = side("tx", phase)
            pick = head_tail[jnp.where(right, 1, 0)]
            z[array * band : (array + 1) * band] = dot(pick, flat).astype(BF16)


def corner_kernel(picks, z0, z1, c0, c1):
    for phase, c in enumerate((c0, c1)):
        down, _ = side("ty", phase)
        pick = picks[jnp.where(down, 1, 0)]
        half = z0.shape[0]
        c[...] = (dot(pick[:, :half], z0[...]) + dot(pick[:, half:], z1[...])).astype(BF16)


def own_kernel(head, scale, q, qd, k, kd, v, vd, qn, qdn, *sums):
    rows, columns, width = q.shape
    count = rows * columns
    pair = pl.program_id(0)
    ones = block_ones(LANES, head.bit_length() - 1, 1.0 / head)

    def flat(ref):
        return ref[...].reshape(count, width)

    query, query_drift = head_pair(flat(q).astype(F32), flat(qd).astype(F32), ones)
    key, key_drift = head_pair(flat(k).astype(F32), flat(kd).astype(F32), ones)
    qn[...] = query
    qdn[...] = query_drift
    place = lax.broadcasted_iota(jnp.int32, (1, count), 1)
    shift = columns.bit_length() - 1
    mask = near(lax.shift_right_logical(place, shift), place & (columns - 1), columns, count)
    factors = [scale[2 * pair + i] / head for i in range(2)]
    parts = attend(query, query_drift, key, key_drift, flat(v), flat(vd), mask, factors, head)
    for ref, part in zip(sums, parts):
        ref[...] = part


def halo_places(places, tile):
    rows, columns = tile
    row, column, group = places[0:1], places[1:2], places[2:3]
    outside = 4 * (rows + columns)
    for phase in range(2):
        down, below = side("ty", phase)
        right, beside = side("tx", phase)
        row_move = jnp.where(below, jnp.where(down, rows, -RADIUS), outside)
        column_move = jnp.where(beside, jnp.where(right, columns, -RADIUS), outside)
        row = row + jnp.where((group & (1 + phase)) != 0, row_move, 0)
        column = column + jnp.where((group & (4 + 4 * phase)) != 0, column_move, 0)
    return row, column


def strip_kernel(head, tile, scale, places, qn, qdn, z0, z1, y0, y1, *sums):
    pair = pl.program_id(0)
    ones = block_ones(LANES, head.bit_length() - 1, 1.0 / head)
    messages = (z0, z1, y0, y1)

    def part(array):
        pieces = []
        for ref in messages:
            size = ref.shape[0] // 4
            pieces.append(ref[array * size : (array + 1) * size])
        return jnp.concatenate(pieces, 0)

    key, key_drift = head_pair(part(0).astype(F32), part(2).astype(F32), ones)
    row, column = halo_places(places, tile)
    mask = near(row, column, tile[1], qn.shape[0])
    factors = [scale[2 * pair + i] / head for i in range(2)]
    parts = attend(
        qn[...], qdn[...], key, key_drift, part(1), part(3), mask, factors, head
    )
    for before, after, piece in zip(sums[:4], sums[4:], parts):
        after[...] = before[...] + piece


def last_kernel(
    head, tile, scale, places, unpack, pool, qn, qdn, c0, c1, a, ce, l, b, weight,
    out, tangent, coarse, running,
):
    pair = pl.program_id(0)
    ones = block_ones(LANES, head.bit_length() - 1, 1.0 / head)

    def part(array):
        pieces = [dot(unpack[array], c[...]) for c in (c0, c1)]
        return jnp.concatenate(pieces, 0)

    key, key_drift = head_pair(part(0), part(2), ones)
    row, column = halo_places(places, tile)
    mask = near(row, column, tile[1], qn.shape[0])
    factors = [scale[2 * pair + i] / head for i in range(2)]
    parts = attend(
        qn[...], qdn[...], key, key_drift, part(1).astype(BF16), part(3).astype(BF16),
        mask, factors, head,
    )
    inverse = 1.0 / (l[...] + parts[2])
    output = (a[...] + parts[0]) * inverse
    moving = (ce[...] + parts[1]) * inverse - output * ((b[...] + parts[3]) * inverse)
    output = output.astype(BF16)
    moving = moving.astype(BF16)
    out[...] = output.reshape(out.shape)
    tangent[...] = moving.reshape(out.shape)
    merged = jnp.concatenate([dot(pool[...], output), dot(pool[...], moving)], 0)
    step = dot(merged.astype(BF16), weight[...])

    @pl.when(pair == 0)
    def _():
        running[...] = step

    @pl.when(pair > 0)
    def _():
        running[...] += step

    @pl.when(pair == pl.num_programs(0) - 1)
    def _():
        coarse[...] = running[...].astype(BF16)


def stacked(refs):
    halves = [ref[...].astype(F32) for ref in refs]
    own = halves[0].shape[0] // 2
    return (
        jnp.concatenate([half[:own] for half in halves], 0),
        jnp.concatenate([half[own:] for half in halves], 0),
    )


def project_kernel(head, slots, mod, weight, *refs):
    tokens, (query_out, keys_out) = refs[:slots], refs[slots:]
    primal, moving = stacked(tokens)
    width = primal.shape[1]
    count = primal.shape[0]
    normed, drift = conditioned(primal, moving, mod, 0, width)
    projected = dot(jnp.concatenate([normed, drift], 0), weight[...])
    span = weight.shape[1] // 3
    ones = block_ones(span, head.bit_length() - 1, 1.0 / head)
    top, low = projected[:count], projected[count:]
    query = head_pair(top[:, :span], low[:, :span], ones)
    key = head_pair(top[:, span : 2 * span], low[:, span : 2 * span], ones)
    query_out[...] = jnp.concatenate(query, 1)
    keys_out[...] = jnp.concatenate(
        [key[0], top[:, 2 * span :].astype(BF16), key[1], low[:, 2 * span :].astype(BF16)], 1
    )


def coarse_kernel(head, slots, groups, scale, weight, query, *refs):
    blocks, outs = refs[:groups], refs[groups:]
    count = query.shape[0]
    span = query.shape[1] // 2
    heads = span // head

    def part(member):
        return jnp.concatenate(
            [block[:, member * span : (member + 1) * span] for block in blocks], 0
        )

    key, value, key_drift, value_drift = (part(member) for member in range(4))
    lane = lax.broadcasted_iota(jnp.int32, (1, span), 1)
    masks = [
        ((lane >= h * head) & (lane < (h + 1) * head)).astype(F32) for h in range(heads)
    ]
    plain, drifting = query[:, :span], query[:, span:]
    plain = jnp.concatenate([plain * mask.astype(BF16) for mask in masks], 0)
    drifting = jnp.concatenate([drifting * mask.astype(BF16) for mask in masks], 0)
    score = dot_nt(plain, key)
    slope = dot_nt(drifting, key) + dot_nt(plain, key_drift)
    weights, tilted = [], []
    for h in range(heads):
        rows = slice(h * count, (h + 1) * count)
        factor = scale[h] / head
        e = jnp.exp2(score[rows] * (factor * LOG2E))
        weights.append(e)
        tilted.append(e * (slope[rows] * factor))
    weights = jnp.concatenate(weights, 0).astype(BF16)
    tilted = jnp.concatenate(tilted, 0).astype(BF16)
    ones = jnp.ones((key.shape[0], span), BF16)

    def own(stack):
        return sum(
            stack[h * count : (h + 1) * count] * mask for h, mask in enumerate(masks)
        )

    inverse = 1.0 / own(dot(weights, ones))
    output = own(dot(weights, value)) * inverse
    shifted = own(dot(tilted, value) + dot(weights, value_drift))
    moving = shifted * inverse - output * (own(dot(tilted, ones)) * inverse)
    both = jnp.concatenate([output.astype(BF16), moving.astype(BF16)], 0)
    spread(dot(both, weight[...]), slots, outs)


def spread(both, slots, outs):
    count = both.shape[0] // 2
    own = count // slots
    for slot, out in enumerate(outs):
        piece = jnp.concatenate(
            [both[slot * own : (slot + 1) * own], both[count + slot * own : count + (slot + 1) * own]],
            0,
        )
        out[...] = piece.astype(out.dtype)


def update_kernel(slots, mod, coarse, *refs):
    parts, (updated, source) = refs[:slots], refs[slots:]
    total = coarse[...].astype(F32)
    for ref in parts:
        total = total + ref[...].astype(F32)
    updated[...] = total
    own, width = total.shape[0] // 2, total.shape[1]
    source[...] = jnp.concatenate(conditioned(total[:own], total[own:], mod, 1, width), 0)


def mlp_kernel(slots, up, down, *refs):
    tokens, outs, running = refs[:slots], refs[slots:-1], refs[-1]
    step = pl.program_id(0)
    primal, moving = stacked(tokens)
    count = primal.shape[0]
    both = jnp.concatenate([primal, moving], 0).astype(BF16)
    hidden = dot(both, up[...])
    x, dx = hidden[:count], hidden[count:]
    root = math.sqrt(2.0 / math.pi)
    square = x * x
    bend = jnp.tanh(root * (x + 0.044715 * (square * x)))
    half = 0.5 * (1.0 + bend)
    rise = half + 0.5 * x * (1.0 - bend * bend) * (root * (1.0 + 3 * 0.044715 * square))
    active = jnp.concatenate([(x * half).astype(BF16), (rise * dx).astype(BF16)], 0)
    result = dot(active, down[...])

    @pl.when(step == 0)
    def _():
        running[...] = result

    @pl.when(step > 0)
    def _():
        running[...] += result

    @pl.when(step == pl.num_programs(0) - 1)
    def _():
        spread(running[...], slots, outs)


def final_kernel(slots, updated, *refs):
    parts, (out, tangent) = refs[:slots], refs[slots:]
    total = updated[...]
    for ref in parts:
        total = total + ref[...].astype(F32)
    own = total.shape[0] // 2
    out[...] = total[:own].astype(BF16).reshape(out.shape)
    tangent[...] = total[own:].astype(BF16).reshape(out.shape)


def modulation(time_plan_index, time_modulation_weight):
    latest = jnp.max(time_plan_index)
    earlier = jnp.min(time_plan_index)
    moment = latest.astype(F32) / STEPS
    spacing = (latest - earlier).astype(F32) / STEPS
    halves = EMBED // 2
    angular = 16.0 ** (jnp.arange(halves).astype(F32) / halves)
    angles = jnp.concatenate([angular * moment, angular * spacing]).reshape(2, halves)
    cosine, sine = jnp.cos(angles), jnp.sin(angles)
    embedded = jnp.stack([cosine, sine], 1)
    slopes = jnp.stack([-angular * sine, angular * cosine], 1)
    features = jnp.stack([embedded.reshape(-1), slopes.reshape(-1)])
    return jnp.dot(features, time_modulation_weight, precision=lax.Precision.HIGHEST)


def struct(shape, dtype=BF16):
    return jax.ShapeDtypeStruct(shape, dtype)


def whole(array):
    return pl.BlockSpec(array.shape, lambda *_: (0,) * len(array.shape))


def smem():
    return pl.BlockSpec(memory_space=pltpu.SMEM)


def columns_of(array, width):
    lead = array.shape[:-1]
    return pl.BlockSpec(lead + (width,), lambda i: (0,) * len(lead) + (i,))


def one_call(kernel, outs, args, smem_count=0, name=None):
    return pl.pallas_call(
        kernel,
        grid=(1,),
        in_specs=[smem()] * smem_count + [whole(a) for a in args[smem_count:]],
        out_specs=[whole(o) for o in outs],
        out_shape=outs,
        name=name,
    )(*args)


def shards(
    queries,
    fine_key_rows,
    fine_value_rows,
    fine_query_tangent,
    fine_key_tangent,
    fine_value_tangent,
    fine_head_scale,
    merged_token_weight,
    time_plan_index,
    time_modulation_weight,
    coarse_projection_weight,
    coarse_head_scale,
    head_output_weight,
    up_projection_weight,
    down_projection_weight,
):
    rows, columns, width = queries.shape
    heads = fine_head_scale.shape[0]
    head = width // heads
    count = rows * columns
    pairs = width // LANES
    tile = (rows, columns)
    strip = RADIUS * columns
    side_tokens = RADIUS * rows
    band = -(-side_tokens // 16) * 16
    square = RADIUS * RADIUS
    corner_keys = 2 * square
    corner_band = -(-corner_keys // 16) * 16
    corner_rows = 4 * corner_keys

    head_tail = np.zeros((2, band, count), np.float32)
    for r in range(rows):
        for c in range(RADIUS):
            head_tail[0, r * RADIUS + c, r * columns + c] = 1
            head_tail[1, r * RADIUS + c, r * columns + columns - RADIUS + c] = 1
    picks = np.zeros((2, corner_rows, 8 * band), np.float32)
    unpack = np.zeros((4, corner_band, corner_rows), np.float32)
    corner_places = np.full((8, 2 * corner_band), 8 * (rows + columns), np.int32)
    corner_places[2:] = 0
    for array in range(4):
        for phase in range(2):
            for r in range(RADIUS):
                for c in range(RADIUS):
                    slot = phase * square + r * RADIUS + c
                    at = array * corner_keys + slot
                    unpack[array, slot, at] = 1
                    for low, first in ((0, 0), (1, rows - RADIUS)):
                        source = phase * 4 * band + array * band + (first + r) * RADIUS + c
                        picks[low, at, source] = 1
                    for meet in range(2):
                        key = meet * corner_band + slot
                        corner_places[:3, key] = (r, c, (1 + meet) + (4 + 4 * phase))
    strip_places = np.full((8, 2 * band + 2 * strip), 8 * (rows + columns), np.int32)
    strip_places[2:] = 0
    for phase in range(2):
        for r in range(rows):
            for c in range(RADIUS):
                strip_places[:3, phase * band + r * RADIUS + c] = (r, c, 4 + 4 * phase)
        for r in range(RADIUS):
            for c in range(columns):
                key = 2 * band + phase * strip + r * columns + c
                strip_places[:3, key] = (r, c, 1 + phase)
    blocks = (rows // MERGE, columns // MERGE)
    own = blocks[0] * blocks[1]
    pool = np.zeros((own, count), np.float32)
    for r in range(rows):
        for c in range(columns):
            pool[(r // MERGE) * blocks[1] + c // MERGE, r * columns + c] = 1 / (MERGE * MERGE)
    head_tail, picks, unpack, pool = (
        jnp.asarray(table, BF16) for table in (head_tail, picks, unpack, pool)
    )
    corner_places, strip_places = jnp.asarray(corner_places), jnp.asarray(strip_places)

    wide = 2 * LANES
    fields = (fine_key_rows, fine_value_rows, fine_key_tangent, fine_value_tangent)
    messages = (
        [struct((4 * strip, width))] * 2 + [struct((4 * band, width))] * 2
    )
    y0, y1, z0, z1 = pl.pallas_call(
        pack_kernel,
        grid=(width // wide,),
        in_specs=[whole(head_tail)] + [columns_of(f, wide) for f in fields],
        out_specs=[columns_of(m, wide) for m in messages],
        out_shape=messages,
        name="pack",
    )(head_tail, *fields)
    down_count, across_count = lax.axis_size("ty"), lax.axis_size("tx")
    y0, y1 = (
        lax.ppermute(y, "ty", couples(down_count, phase)) for phase, y in enumerate((y0, y1))
    )
    z0, z1 = (
        lax.ppermute(z, "tx", couples(across_count, phase)) for phase, z in enumerate((z0, z1))
    )

    flat = struct((count, width))
    sums = [struct((count, width), F32)] * 4
    fine = (
        queries, fine_query_tangent, fine_key_rows, fine_key_tangent, fine_value_rows,
        fine_value_tangent,
    )
    qn, qdn, *own_sums = pl.pallas_call(
        functools.partial(own_kernel, head),
        grid=(pairs,),
        in_specs=[smem()] + [columns_of(f, LANES) for f in fine],
        out_specs=[columns_of(o, LANES) for o in [flat] * 2 + sums],
        out_shape=[flat] * 2 + sums,
        name="own_attention",
    )(fine_head_scale, *fine)

    corner = struct((corner_rows, width))
    c0, c1 = pl.pallas_call(
        corner_kernel,
        grid=(width // wide,),
        in_specs=[whole(picks)] + [columns_of(z, wide) for z in (z0, z1)],
        out_specs=[columns_of(corner, wide)] * 2,
        out_shape=[corner] * 2,
        name="corners",
    )(picks, z0, z1)
    c0, c1 = (
        lax.ppermute(c, "ty", couples(down_count, phase)) for phase, c in enumerate((c0, c1))
    )
    strip_args = (qn, qdn, z0, z1, y0, y1, *own_sums)
    strip_sums = pl.pallas_call(
        functools.partial(strip_kernel, head, tile),
        grid=(pairs,),
        in_specs=[smem(), whole(strip_places)] + [columns_of(a, LANES) for a in strip_args],
        out_specs=[columns_of(o, LANES) for o in sums],
        out_shape=sums,
        input_output_aliases={8 + i: i for i in range(4)},
        name="strip_attention",
    )(fine_head_scale, strip_places, *strip_args)
    last_args = (qn, qdn, c0, c1, *strip_sums)
    grid_shape = struct(queries.shape)
    pooled = struct((2 * own, width))
    fine_out, fine_tangent, coarse = pl.pallas_call(
        functools.partial(last_kernel, head, tile),
        grid=(pairs,),
        in_specs=[smem()]
        + [whole(t) for t in (corner_places, unpack, pool)]
        + [columns_of(a, LANES) for a in last_args]
        + [pl.BlockSpec((LANES, width), lambda i: (i, 0))],
        out_specs=[columns_of(grid_shape, LANES)] * 2 + [whole(pooled)],
        out_shape=[grid_shape] * 2 + [pooled],
        scratch_shapes=[pltpu.VMEM((2 * own, width), F32)],
        name="last_attention",
    )(fine_head_scale, corner_places, unpack, pool, *last_args, merged_token_weight)

    mod = modulation(time_plan_index, time_modulation_weight)
    near_heads = coarse_head_scale.shape[0]
    span = near_heads * head
    packed = (
        coarse_projection_weight.reshape(width, near_heads, 3, head)
        .transpose(0, 2, 1, 3)
        .reshape(width, 3 * span)
    )
    slots = across_count
    tokens = gathered(coarse, "tx")
    group = slots * own
    query, keys = one_call(
        functools.partial(project_kernel, head, slots),
        [struct((group, 2 * span)), struct((group, 4 * span))],
        (mod, packed, *tokens),
        name="project",
    )
    key_blocks = gathered(keys, "ty")
    pieces = [struct((2 * own, width), F32)] + [struct((2 * own, width))] * (slots - 1)
    kept, *sent = one_call(
        functools.partial(coarse_kernel, head, slots, down_count),
        pieces,
        (coarse_head_scale, head_output_weight.reshape(span, width), query, *key_blocks),
        1,
        name="coarse_attention",
    )
    updated, source = one_call(
        functools.partial(update_kernel, slots),
        [struct((2 * own, width), F32), struct((2 * own, width))],
        (mod, coarse, kept, *returned(sent, "tx")),
        name="update",
    )
    sources = gathered(source, "tx")
    units = up_projection_weight.shape[1]
    step = min(units, wide)
    kept, *sent = pl.pallas_call(
        functools.partial(mlp_kernel, slots),
        grid=(units // step,),
        in_specs=[
            pl.BlockSpec((width, step), lambda i: (0, i)),
            pl.BlockSpec((step, width), lambda i: (i, 0)),
        ]
        + [whole(s) for s in sources],
        out_specs=[whole(p) for p in pieces],
        out_shape=pieces,
        scratch_shapes=[pltpu.VMEM((2 * group, width), F32)],
        name="mlp",
    )(up_projection_weight, down_projection_weight, *sources)
    block_shape = struct((*blocks, width))
    coarse_out, coarse_tangent = one_call(
        functools.partial(final_kernel, slots),
        [block_shape] * 2,
        (updated, kept, *returned(sent, "tx")),
        name="final",
    )
    return (fine_out, fine_tangent, coarse_out, coarse_tangent)


def solution(mesh):
    return jax.shard_map(
        shards,
        mesh=mesh,
        in_specs=(
            P("ty", "tx", None),
            P("ty", "tx", None),
            P("ty", "tx", None),
            P("ty", "tx", None),
            P("ty", "tx", None),
            P("ty", "tx", None),
            P(),
            P(),
            P(),
            P(),
            P(None, "tx", None),
            P("tx"),
            P("tx", None, None),
            P(None, "tx"),
            P("tx", None),
        ),
        out_specs=(
            P("ty", "tx", None),
            P("ty", "tx", None),
            P("ty", "tx", None),
            P("ty", "tx", None),
        ),
        check_vma=False,
    )
```

```python
import functools
import math

import jax
import jax.numpy as jnp
from jax import lax
from jax.experimental import pallas as pl
from jax.experimental.pallas import tpu as pltpu
from jax.sharding import PartitionSpec as P

EMBED = 128
RADIUS = 3
MERGE = 4
STEPS = 1000
EPSILON = 1e-06
LANES = 128
TOGETHER = 4
LOG2E = math.log2(math.e)
F32 = jnp.float32
BF16 = jnp.bfloat16


def dot(a, b):
    return jnp.dot(a, b, preferred_element_type=F32)


def dot_nt(a, b):
    return lax.dot_general(a, b, (((1,), (1,)), ((), ())), preferred_element_type=F32)


def block_ones(width, head, value):
    row = lax.broadcasted_iota(jnp.int32, (width, width), 0)
    col = lax.broadcasted_iota(jnp.int32, (width, width), 1)
    same = lax.shift_right_logical(row, head) == lax.shift_right_logical(col, head)
    return jnp.where(same, value, 0.0).astype(BF16)


def head_means(arrays, ones):
    highs = [array.astype(BF16) for array in arrays]
    lows = [(a - h.astype(F32)).astype(BF16) for a, h in zip(arrays, highs)]
    means = dot(jnp.concatenate(highs, 0), ones) + dot(jnp.concatenate(lows, 0), ones)
    pieces, at = [], 0
    for array in arrays:
        pieces.append(means[at : at + array.shape[0]])
        at += array.shape[0]
    return pieces


def head_pairs(couples_of, ones):
    factors = [
        lax.rsqrt(mean + EPSILON)
        for mean in head_means([values * values for values, _ in couples_of], ones)
    ]
    normed = [values * factor for (values, _), factor in zip(couples_of, factors)]
    leans = head_means([n * tangent for n, (_, tangent) in zip(normed, couples_of)], ones)
    return [
        (n.astype(BF16), ((tangent - n * lean) * factor).astype(BF16))
        for n, (_, tangent), lean, factor in zip(normed, couples_of, leans, factors)
    ]


def row_pair(values, tangent):
    factor = lax.rsqrt(jnp.mean(values * values, axis=-1, keepdims=True) + EPSILON)
    normed = values * factor
    drift = (tangent - normed * jnp.mean(normed * tangent, axis=-1, keepdims=True)) * factor
    return normed, drift


def conditioned(values, tangent, mod, part, width):
    normed, drift = row_pair(values, tangent)
    offset = mod[0:1, 2 * part * width : (2 * part + 1) * width]
    stretch = mod[0:1, (2 * part + 1) * width : (2 * part + 2) * width]
    offset_drift = mod[1:2, 2 * part * width : (2 * part + 1) * width]
    stretch_drift = mod[1:2, (2 * part + 1) * width : (2 * part + 2) * width]
    primal = (normed * (1.0 + stretch) + offset).astype(BF16)
    moving = (drift * (1.0 + stretch) + normed * stretch_drift + offset_drift).astype(BF16)
    return primal, moving


def side(axis, phase):
    at = lax.axis_index(axis)
    after = (at & 1) == phase
    exists = jnp.where(after, at + 1 < lax.axis_size(axis), at > 0)
    return after, exists


def couples(count, phase):
    return [
        edge for i in range(phase, count - 1, 2) for edge in ((i, i + 1), (i + 1, i))
    ]


def partner(count, step, back=False):
    if count & (count - 1) == 0:
        return [(i, i ^ step) for i in range(count)]
    return [(i, (i - step if back else i + step) % count) for i in range(count)]


def gathered(value, axis):
    count = lax.axis_size(axis)
    return [value] + [
        lax.ppermute(value, axis, partner(count, step)) for step in range(1, count)
    ]


def row_gathered(value, axis):
    count = lax.axis_size(axis)
    if count < 4 or count & (count - 1):
        return gathered(value, axis)
    part = jnp.concatenate(
        [value] + [lax.ppermute(value, axis, partner(count, step)) for step in range(2, count, 2)],
        0,
    )
    return [part, lax.ppermute(part, axis, partner(count, 1))]


def returned(pieces, axis):
    count = lax.axis_size(axis)
    return [
        lax.ppermute(piece, axis, partner(count, step, True))
        for step, piece in zip(range(1, count), pieces)
    ]


def attend(items, mask, head):
    count, keys = mask.shape
    lane = lax.broadcasted_iota(jnp.int32, (1, LANES), 1)
    first = (lane < head).astype(F32).astype(BF16)
    second = (lane >= head).astype(F32).astype(BF16)
    scores, slopes = [], []
    for query, query_drift, key, key_drift, _, _, _ in items:
        query_0, query_1 = query * first, query * second
        drift_0, drift_1 = query_drift * first, query_drift * second
        scores.append(dot_nt(jnp.concatenate([query_0, query_1], 0), key))
        slopes.append(
            dot_nt(
                jnp.concatenate(
                    [
                        jnp.concatenate([drift_0, query_0], 1),
                        jnp.concatenate([drift_1, query_1], 1),
                    ],
                    0,
                ),
                jnp.concatenate([key, key_drift], 1),
            )
        )
    weights, tilts = [], []
    for score, slope, item in zip(scores, slopes, items):
        heavy, tilted = [], []
        for place, factor in enumerate(item[6]):
            rows = slice(place * count, (place + 1) * count)
            weight = jnp.exp2(score[rows] * (factor * LOG2E)) * mask
            heavy.append(weight.astype(BF16))
            tilted.append((weight * (slope[rows] * factor)).astype(BF16))
        weights.append(jnp.concatenate(heavy, 0))
        tilts.append(jnp.concatenate(tilted, 0))
    ones = jnp.ones((keys, LANES), BF16)

    def own(stack):
        return jnp.where(lane < head, stack[:count], stack[count:])

    results = []
    for weight, tilt, item in zip(weights, tilts, items):
        value, value_drift = item[4], item[5]
        mixed = dot(weight, jnp.concatenate([value, value_drift], 1))
        turned = dot(tilt, value)
        sums = dot(jnp.concatenate([weight, tilt], 0), ones)
        results.append(
            (
                own(mixed[:, :LANES]),
                own(mixed[:, LANES:] + turned),
                own(sums[: 2 * count]),
                own(sums[2 * count :]),
            )
        )
    return results


def near(key_row, key_column, columns, count):
    place = lax.broadcasted_iota(jnp.int32, (count, 1), 0)
    shift = columns.bit_length() - 1
    row = lax.shift_right_logical(place, shift)
    column = place & (columns - 1)
    close = (jnp.abs(row - key_row) <= RADIUS) & (jnp.abs(column - key_column) <= RADIUS)
    return jnp.where(close, 1.0, 0.0)


def one_hot(rows, place, valid):
    row = lax.broadcasted_iota(jnp.int32, (rows, place.shape[1]), 0)
    return jnp.where((row == place) & valid, 1.0, 0.0).astype(BF16)


def log2(number):
    return number.bit_length() - 1


def by_radius(number):
    return lax.shift_right_logical(number * (128 // RADIUS + 1), 7)


def pack_kernel(key, value, key_drift, value_drift, query, query_drift, *refs):
    y0, y1, z0, z1, sems = *refs[:4], refs[-1]
    near = refs[4:10]
    far = (key, value, key_drift, value_drift, query, query_drift)
    copies = [
        pltpu.make_async_copy(source, target, sems.at[i])
        for i, (source, target) in enumerate(zip(far, near))
    ]
    for copy in copies:
        copy.start()
    rows, columns, width = key.shape
    count = rows * columns
    strip = RADIUS * columns
    band = z0.shape[0] // 4
    place = lax.broadcasted_iota(jnp.int32, (1, count), 1)
    row = lax.shift_right_logical(place, log2(columns))
    picks, starts = [], []
    for phase in range(2):
        right, _ = side("tx", phase)
        column = (place & (columns - 1)) - jnp.where(right, columns - RADIUS, 0)
        valid = (column >= 0) & (column < RADIUS)
        picks.append(one_hot(band, row * RADIUS + column, valid))
        down, _ = side("ty", phase)
        starts.append(jnp.where(down, rows - RADIUS, 0))
    for array, ref in enumerate(near[:4]):
        copies[array].wait()
        flat = ref[...].reshape(count, width)
        for start, pick, y, z in zip(starts, picks, (y0, y1), (z0, z1)):
            y[array * strip : (array + 1) * strip] = ref[pl.ds(start, RADIUS)].reshape(
                strip, width
            )
            z[array * band : (array + 1) * band] = dot(pick, flat).astype(BF16)
    for copy in copies[4:]:
        copy.wait()


def corner_kernel(rows, z0, z1, c0, c1):
    half = z0.shape[0]
    band = half // 4
    square = RADIUS * RADIUS
    place = lax.broadcasted_iota(jnp.int32, (1, half), 1)
    array = lax.shift_right_logical(place, log2(band))
    for phase, c in enumerate((c0, c1)):
        down, _ = side("ty", phase)
        token = (place & (band - 1)) - jnp.where(down, (rows - RADIUS) * RADIUS, 0)
        valid = (token >= 0) & (token < square)
        total = None
        for meet, z in enumerate((z0, z1)):
            at = (2 * array + meet) * square + token
            part = dot(one_hot(c.shape[0], at, valid), z[...])
            total = part if total is None else total + part
        c[...] = total.astype(BF16)


def each_group(pairs, body):
    together = math.gcd(pairs, TOGETHER)

    @pl.loop(0, pairs // together)
    def _(step):
        starts = [
            pl.multiple_of((step * together + i) * LANES, LANES) for i in range(together)
        ]
        body(step * together, [pl.ds(start, LANES) for start in starts])


def own_kernel(head, scale, q, qd, k, kd, v, vd, qn, qdn, *sums):
    rows, columns, width = q.shape
    count = rows * columns
    ones = block_ones(LANES, head.bit_length() - 1, 1.0 / head)
    place = lax.broadcasted_iota(jnp.int32, (1, count), 1)
    shift = columns.bit_length() - 1
    mask = near(lax.shift_right_logical(place, shift), place & (columns - 1), columns, count)

    def body(pair, lanes):
        def flat(ref, at):
            return ref[:, :, at].reshape(count, LANES)

        normed = head_pairs(
            [
                (flat(a, at).astype(F32), flat(b, at).astype(F32))
                for at in lanes
                for a, b in ((q, qd), (k, kd))
            ],
            ones,
        )
        items = []
        for i, at in enumerate(lanes):
            query, key = normed[2 * i], normed[2 * i + 1]
            qn[:, at], qdn[:, at] = query
            factors = [scale[2 * (pair + i) + j] / head for j in range(2)]
            items.append((*query, *key, flat(v, at), flat(vd, at), factors))
        for at, parts in zip(lanes, attend(items, mask, head)):
            for ref, part in zip(sums, parts):
                ref[:, at] = part

    each_group(width // LANES, body)


def moved(row, column, phase_down, phase_right, tile):
    rows, columns = tile
    outside = 4 * (rows + columns)
    for phase in range(2):
        down, below = side("ty", phase)
        right, beside = side("tx", phase)
        row_move = jnp.where(below, jnp.where(down, rows, -RADIUS), outside)
        column_move = jnp.where(beside, jnp.where(right, columns, -RADIUS), outside)
        row = row + jnp.where(phase_down == phase, row_move, 0)
        column = column + jnp.where(phase_right == phase, column_move, 0)
    return row, column


def strip_places(tile, band):
    rows, columns = tile
    strip = RADIUS * columns
    place = lax.broadcasted_iota(jnp.int32, (1, 2 * band + 2 * strip), 1)
    beside = place < 2 * band
    phase = lax.shift_right_logical(place, log2(band))
    token = place & (band - 1)
    side_row = by_radius(token)
    side_column = token - side_row * RADIUS
    side_row = jnp.where(side_row < rows, side_row, 8 * (rows + columns))
    rest = place - 2 * band
    later = rest >= strip
    rest = rest - jnp.where(later, strip, 0)
    row = jnp.where(beside, side_row, lax.shift_right_logical(rest, log2(columns)))
    column = jnp.where(beside, side_column, rest & (columns - 1))
    down = jnp.where(beside, -1, jnp.where(later, 1, 0))
    return moved(row, column, down, jnp.where(beside, phase, -1), tile)


def corner_places(tile, band):
    square = RADIUS * RADIUS
    place = lax.broadcasted_iota(jnp.int32, (1, 2 * band), 1)
    slot = place & (band - 1)
    later = slot >= square
    token = slot - jnp.where(later, square, 0)
    row = by_radius(token)
    column = token - row * RADIUS
    row = jnp.where(slot < 2 * square, row, 8 * sum(tile))
    down = lax.shift_right_logical(place, log2(band))
    return moved(row, column, down, jnp.where(later, 1, 0), tile)


def strip_kernel(head, tile, scale, qn, qdn, z0, z1, y0, y1, *sums):
    ones = block_ones(LANES, head.bit_length() - 1, 1.0 / head)
    messages = (z0, z1, y0, y1)
    row, column = strip_places(tile, z0.shape[0] // 4)
    mask = near(row, column, tile[1], qn.shape[0])

    def body(pair, lanes):
        def part(array, at):
            pieces = []
            for ref in messages:
                size = ref.shape[0] // 4
                pieces.append(ref[array * size : (array + 1) * size, at])
            return jnp.concatenate(pieces, 0)

        keys = head_pairs(
            [(part(0, at).astype(F32), part(2, at).astype(F32)) for at in lanes], ones
        )
        items = [
            (
                qn[:, at], qdn[:, at], *key, part(1, at), part(3, at),
                [scale[2 * (pair + i) + j] / head for j in range(2)],
            )
            for i, (at, key) in enumerate(zip(lanes, keys))
        ]
        for at, parts in zip(lanes, attend(items, mask, head)):
            for before, after, piece in zip(sums[:4], sums[4:], parts):
                after[:, at] = before[:, at] + piece

    each_group(qn.shape[1] // LANES, body)


def last_kernel(
    head, tile, scale, qn, qdn, c0, c1, a, ce, l, b, weight, out, tangent, coarse, pooled
):
    rows, columns = tile
    count = rows * columns
    ones = block_ones(LANES, log2(head), 1.0 / head)
    corner_rows = c0.shape[0]
    corner_keys = corner_rows // 4
    band = -(-corner_keys // 32) * 32
    row, column = corner_places(tile, band)
    mask = near(row, column, columns, count)
    place = lax.broadcasted_iota(jnp.int32, (1, corner_rows), 1)
    unpack = []
    for array in range(4):
        slot = place - array * corner_keys
        unpack.append(one_hot(band, slot, (slot >= 0) & (slot < corner_keys)))
    own = pooled.shape[0] // 2
    place = lax.broadcasted_iota(jnp.int32, (1, count), 1)
    block = lax.shift_right_logical(place, log2(columns) + log2(MERGE)) * (columns // MERGE)
    block = block + lax.shift_right_logical(place & (columns - 1), log2(MERGE))
    pool = one_hot(own, block, block >= 0) * jnp.asarray(1 / (MERGE * MERGE), BF16)

    def body(pair, lanes):
        def part(array, at):
            return jnp.concatenate([dot(unpack[array], c[:, at]) for c in (c0, c1)], 0)

        keys = head_pairs([(part(0, at), part(2, at)) for at in lanes], ones)
        items = [
            (
                qn[:, at], qdn[:, at], *key, part(1, at).astype(BF16),
                part(3, at).astype(BF16),
                [scale[2 * (pair + i) + j] / head for j in range(2)],
            )
            for i, (at, key) in enumerate(zip(lanes, keys))
        ]
        for at, parts in zip(lanes, attend(items, mask, head)):
            inverse = 1.0 / (l[:, at] + parts[2])
            output = (a[:, at] + parts[0]) * inverse
            moving = (ce[:, at] + parts[1]) * inverse - output * ((b[:, at] + parts[3]) * inverse)
            output = output.astype(BF16)
            moving = moving.astype(BF16)
            out[:, :, at] = output.reshape(*tile, LANES)
            tangent[:, :, at] = moving.reshape(*tile, LANES)
            pooled[:own, at] = dot(pool, output)
            pooled[own:, at] = dot(pool, moving)

    each_group(qn.shape[1] // LANES, body)
    coarse[...] = dot(pooled[...].astype(BF16), weight[...]).astype(BF16)


def stacked(refs):
    halves = [ref[...].astype(F32) for ref in refs]
    own = halves[0].shape[0] // 2
    return (
        jnp.concatenate([half[:own] for half in halves], 0),
        jnp.concatenate([half[own:] for half in halves], 0),
    )


def project_kernel(head, slots, mod, weight, *refs):
    tokens, (query_out, keys_out) = refs[:slots], refs[slots:]
    primal, moving = stacked(tokens)
    width = primal.shape[1]
    count = primal.shape[0]
    both = jnp.concatenate(conditioned(primal, moving, mod, 0, width), 0)
    heads = weight.shape[0] // (3 * head)
    span = heads * head
    ones = block_ones(span, head.bit_length() - 1, 1.0 / head)

    def projected(member):
        rows = [weight[(3 * h + member) * head : (3 * h + member + 1) * head] for h in range(heads)]
        result = dot_nt(both, jnp.concatenate(rows, 0))
        return result[:count], result[count:]

    query, key = head_pairs([projected(0), projected(1)], ones)
    value, value_drift = projected(2)
    query_out[...] = jnp.concatenate(query, 1)
    keys_out[...] = jnp.concatenate(
        [key[0], value.astype(BF16), key[1], value_drift.astype(BF16)], 1
    )


def coarse_kernel(head, slots, groups, scale, weight, query, *refs):
    blocks, outs = refs[:groups], refs[groups:]
    count = query.shape[0]
    span = query.shape[1] // 2
    heads = span // head

    def part(member):
        return jnp.concatenate(
            [block[:, member * span : (member + 1) * span] for block in blocks], 0
        )

    key, value, key_drift, value_drift = (part(member) for member in range(4))
    lane = lax.broadcasted_iota(jnp.int32, (1, span), 1)
    masks = [
        ((lane >= h * head) & (lane < (h + 1) * head)).astype(F32) for h in range(heads)
    ]
    plain, drifting = query[:, :span], query[:, span:]
    plain = jnp.concatenate([plain * mask.astype(BF16) for mask in masks], 0)
    drifting = jnp.concatenate([drifting * mask.astype(BF16) for mask in masks], 0)
    score = dot_nt(plain, key)
    slope = dot_nt(drifting, key) + dot_nt(plain, key_drift)
    weights, tilted = [], []
    for h in range(heads):
        rows = slice(h * count, (h + 1) * count)
        factor = scale[h] / head
        e = jnp.exp2(score[rows] * (factor * LOG2E))
        weights.append(e)
        tilted.append(e * (slope[rows] * factor))
    weights = jnp.concatenate(weights, 0).astype(BF16)
    tilted = jnp.concatenate(tilted, 0).astype(BF16)
    ones = jnp.ones((key.shape[0], span), BF16)

    def own(stack):
        return sum(
            stack[h * count : (h + 1) * count] * mask for h, mask in enumerate(masks)
        )

    inverse = 1.0 / own(dot(weights, ones))
    output = own(dot(weights, value)) * inverse
    shifted = own(dot(tilted, value) + dot(weights, value_drift))
    moving = shifted * inverse - output * (own(dot(tilted, ones)) * inverse)
    both = jnp.concatenate([output.astype(BF16), moving.astype(BF16)], 0)
    spread(dot(both, weight[...]), slots, outs)


def spread(both, slots, outs):
    count = both.shape[0] // 2
    own = count // slots
    for slot, out in enumerate(outs):
        piece = jnp.concatenate(
            [both[slot * own : (slot + 1) * own], both[count + slot * own : count + (slot + 1) * own]],
            0,
        )
        out[...] = piece.astype(out.dtype)


def update_kernel(slots, mod, coarse, *refs):
    parts, (updated, source) = refs[:slots], refs[slots:]
    total = coarse[...].astype(F32)
    for ref in parts:
        total = total + ref[...].astype(F32)
    updated[...] = total
    own, width = total.shape[0] // 2, total.shape[1]
    source[...] = jnp.concatenate(conditioned(total[:own], total[own:], mod, 1, width), 0)


def mlp_kernel(slots, up, down, *refs):
    tokens, outs = refs[:slots], refs[slots:]
    primal, moving = stacked(tokens)
    count = primal.shape[0]
    both = jnp.concatenate([primal, moving], 0).astype(BF16)
    hidden = dot(both, up[...])
    x, dx = hidden[:count], hidden[count:]
    root = math.sqrt(2.0 / math.pi)
    square = x * x
    bend = jnp.tanh(root * (x + 0.044715 * (square * x)))
    half = 0.5 * (1.0 + bend)
    rise = half + 0.5 * x * (1.0 - bend * bend) * (root * (1.0 + 3 * 0.044715 * square))
    active = jnp.concatenate([(x * half).astype(BF16), (rise * dx).astype(BF16)], 0)
    spread(dot(active, down[...]), slots, outs)


def final_kernel(slots, updated, *refs):
    parts, (out, tangent) = refs[:slots], refs[slots:]
    total = updated[...]
    for ref in parts:
        total = total + ref[...].astype(F32)
    own = total.shape[0] // 2
    out[...] = total[:own].astype(BF16).reshape(out.shape)
    tangent[...] = total[own:].astype(BF16).reshape(out.shape)


def modulation_kernel(index, weight, out):
    latest = jnp.maximum(index[0], index[1])
    earlier = jnp.minimum(index[0], index[1])
    halves = EMBED // 2
    row = lax.broadcasted_iota(jnp.int32, (2 * EMBED, LANES), 0)
    angular = jnp.exp2((row & (halves - 1)).astype(F32) * (4.0 / halves))
    steps = jnp.where(row < EMBED, latest, latest - earlier).astype(F32) / STEPS
    angle = angular * steps
    cosine, sine = jnp.cos(angle), jnp.sin(angle)
    even = (row & halves) == 0
    feature = jnp.where(even, cosine, sine)
    slope = jnp.where(even, -sine, cosine) * angular

    @pl.loop(0, weight.shape[1] // LANES)
    def _(step):
        at = pl.ds(pl.multiple_of(step * LANES, LANES), LANES)
        block = weight[:, at]
        out[0:1, at] = jnp.sum(feature * block, axis=0, keepdims=True)
        out[1:2, at] = jnp.sum(slope * block, axis=0, keepdims=True)


def struct(shape, dtype=BF16):
    return jax.ShapeDtypeStruct(shape, dtype)


def near_call(kernel, outs, args, smem_count=0, scratch=(), name=None, far_out=False):
    def near_spec():
        return pl.BlockSpec(memory_space=pltpu.VMEM)

    args = [
        a if i < smem_count else pltpu.with_memory_space_constraint(a, pltpu.VMEM)
        for i, a in enumerate(args)
    ]
    return pl.pallas_call(
        kernel,
        in_specs=[pl.BlockSpec(memory_space=pltpu.SMEM)] * smem_count
        + [near_spec()] * (len(args) - smem_count),
        out_specs=[pl.BlockSpec() if far_out else near_spec() for _ in outs],
        out_shape=outs if far_out else [pltpu.VMEM(o.shape, o.dtype) for o in outs],
        scratch_shapes=list(scratch),
        compiler_params=pltpu.CompilerParams(vmem_limit_bytes=16 * 1024 * 1024),
        name=name,
    )(*args)


def shards(
    queries,
    fine_key_rows,
    fine_value_rows,
    fine_query_tangent,
    fine_key_tangent,
    fine_value_tangent,
    fine_head_scale,
    merged_token_weight,
    time_plan_index,
    time_modulation_weight,
    coarse_projection_weight,
    coarse_head_scale,
    head_output_weight,
    up_projection_weight,
    down_projection_weight,
):
    rows, columns, width = queries.shape
    heads = fine_head_scale.shape[0]
    head = width // heads
    count = rows * columns
    pairs = width // LANES
    tile = (rows, columns)
    strip = RADIUS * columns
    side_tokens = RADIUS * rows
    band = 1 << (max(side_tokens, 16) - 1).bit_length()
    corner_rows = 8 * RADIUS * RADIUS
    blocks = (rows // MERGE, columns // MERGE)
    own = blocks[0] * blocks[1]

    fields = (fine_key_rows, fine_value_rows, fine_key_tangent, fine_value_tangent)
    near = pl.BlockSpec(memory_space=pltpu.VMEM)
    messages = [pltpu.VMEM((4 * strip, width), BF16)] * 2
    messages += [pltpu.VMEM((4 * band, width), BF16)] * 2
    y0, y1, z0, z1, *fine = pl.pallas_call(
        pack_kernel,
        in_specs=[pl.BlockSpec(memory_space=pltpu.HBM)] * 6,
        out_specs=[near] * 10,
        out_shape=messages + [pltpu.VMEM(queries.shape, BF16)] * 6,
        scratch_shapes=[pltpu.SemaphoreType.DMA((6,))],
        compiler_params=pltpu.CompilerParams(vmem_limit_bytes=16 * 1024 * 1024),
        name="pack",
    )(
        *(
            pltpu.with_memory_space_constraint(field, pltpu.HBM)
            for field in (
                fine_key_rows, fine_value_rows, fine_key_tangent, fine_value_tangent,
                queries, fine_query_tangent,
            )
        )
    )
    key, value, key_drift, value_drift, query, query_drift = fine
    down_count, across_count = lax.axis_size("ty"), lax.axis_size("tx")
    y0, y1 = (
        lax.ppermute(y, "ty", couples(down_count, phase)) for phase, y in enumerate((y0, y1))
    )
    z0, z1 = (
        lax.ppermute(z, "tx", couples(across_count, phase)) for phase, z in enumerate((z0, z1))
    )

    flat = struct((count, width))
    sums = [struct((count, width), F32)] * 4
    qn, qdn, *own_sums = near_call(
        functools.partial(own_kernel, head),
        [flat] * 2 + sums,
        (
            fine_head_scale, query, query_drift, key, key_drift, value, value_drift,
        ),
        1,
        name="own_attention",
    )
    z0, z1, qn = lax.optimization_barrier((z0, z1, qn))
    corner = struct((corner_rows, width))
    c0, c1 = near_call(
        functools.partial(corner_kernel, rows), [corner] * 2, (z0, z1), name="corners"
    )
    c0, c1 = (
        lax.ppermute(c, "ty", couples(down_count, phase)) for phase, c in enumerate((c0, c1))
    )
    strip_sums = near_call(
        functools.partial(strip_kernel, head, tile),
        sums,
        (fine_head_scale, qn, qdn, z0, z1, y0, y1, *own_sums),
        1,
        name="strip_attention",
    )
    grid_shape = struct(queries.shape)
    pooled = struct((2 * own, width))
    fine_out, fine_tangent, coarse = near_call(
        functools.partial(last_kernel, head, tile),
        [grid_shape] * 2 + [pooled],
        (
            fine_head_scale, qn, qdn, c0, c1, *strip_sums, merged_token_weight,
        ),
        1,
        [pltpu.VMEM((2 * own, width), F32)],
        name="last_attention",
    )

    (mod,) = near_call(
        modulation_kernel,
        [struct((2, 4 * width), F32)],
        (time_plan_index, time_modulation_weight),
        1,
        name="modulation",
    )
    near_heads = coarse_head_scale.shape[0]
    span = near_heads * head
    packed = coarse_projection_weight.transpose(1, 2, 0).reshape(3 * span, width)
    slots = across_count
    tokens = gathered(coarse, "tx")
    group = slots * own
    query, keys = near_call(
        functools.partial(project_kernel, head, slots),
        [struct((group, 2 * span)), struct((group, 4 * span))],
        (mod, packed, *tokens),
        name="project",
    )
    key_blocks = row_gathered(keys, "ty")
    pieces = [struct((2 * own, width), F32)] + [struct((2 * own, width))] * (slots - 1)
    kept, *sent = near_call(
        functools.partial(coarse_kernel, head, slots, len(key_blocks)),
        pieces,
        (coarse_head_scale, head_output_weight.reshape(span, width), query, *key_blocks),
        1,
        name="coarse_attention",
    )
    updated, source = near_call(
        functools.partial(update_kernel, slots),
        [struct((2 * own, width), F32), struct((2 * own, width))],
        (mod, coarse, kept, *returned(sent, "tx")),
        name="update",
    )
    kept, *sent = near_call(
        functools.partial(mlp_kernel, slots),
        pieces,
        (up_projection_weight, down_projection_weight, *gathered(source, "tx")),
        name="mlp",
    )
    coarse_out, coarse_tangent = near_call(
        functools.partial(final_kernel, slots),
        [struct((*blocks, width))] * 2,
        (updated, kept, *returned(sent, "tx")),
        name="final",
        far_out=True,
    )
    return (fine_out, fine_tangent, coarse_out, coarse_tangent)


def solution(mesh):
    return jax.shard_map(
        shards,
        mesh=mesh,
        in_specs=(
            P("ty", "tx", None),
            P("ty", "tx", None),
            P("ty", "tx", None),
            P("ty", "tx", None),
            P("ty", "tx", None),
            P("ty", "tx", None),
            P(),
            P(),
            P(),
            P(),
            P(None, "tx", None),
            P("tx"),
            P("tx", None, None),
            P(None, "tx"),
            P("tx", None),
        ),
        out_specs=(
            P("ty", "tx", None),
            P("ty", "tx", None),
            P("ty", "tx", None),
            P("ty", "tx", None),
        ),
        check_vma=False,
    )
```

```python
import functools
import math

import jax
import jax.numpy as jnp
from jax import lax
from jax.experimental import pallas as pl
from jax.experimental.pallas import tpu as pltpu
from jax.sharding import PartitionSpec as P


EMBED = 128
RADIUS = 3
MERGE = 4
STEPS = 1000
EPSILON = 1e-06
LANES = 128
WIDE = 256
LOG2E = math.log2(math.e)
F32 = jnp.float32
BF16 = jnp.bfloat16


def dot(a, b):
    return jnp.dot(a, b, preferred_element_type=F32)


def dot_nt(a, b):
    return lax.dot_general(a, b, (((1,), (1,)), ((), ())), preferred_element_type=F32)


def block_ones(width, head, value):
    row = lax.broadcasted_iota(jnp.int32, (width, width), 0)
    col = lax.broadcasted_iota(jnp.int32, (width, width), 1)
    same = lax.shift_right_logical(row, head) == lax.shift_right_logical(col, head)
    return jnp.where(same, value, 0.0).astype(BF16)


def head_means(arrays, ones):
    highs = [array.astype(BF16) for array in arrays]
    lows = [(a - h.astype(F32)).astype(BF16) for a, h in zip(arrays, highs)]
    means = dot(jnp.concatenate(highs, 0), ones) + dot(jnp.concatenate(lows, 0), ones)
    pieces, at = [], 0
    for array in arrays:
        pieces.append(means[at : at + array.shape[0]])
        at += array.shape[0]
    return pieces


def head_pairs(couples_of, ones):
    factors = [
        lax.rsqrt(mean + EPSILON)
        for mean in head_means([values * values for values, _ in couples_of], ones)
    ]
    normed = [values * factor for (values, _), factor in zip(couples_of, factors)]
    leans = head_means([n * tangent for n, (_, tangent) in zip(normed, couples_of)], ones)
    return [
        (n.astype(BF16), ((tangent - n * lean) * factor).astype(BF16))
        for n, (_, tangent), lean, factor in zip(normed, couples_of, leans, factors)
    ]


def row_pair(values, tangent):
    factor = lax.rsqrt(jnp.mean(values * values, axis=-1, keepdims=True) + EPSILON)
    normed = values * factor
    drift = (tangent - normed * jnp.mean(normed * tangent, axis=-1, keepdims=True)) * factor
    return normed, drift


def conditioned(values, tangent, mod, part, width):
    normed, drift = row_pair(values, tangent)
    offset = mod[0:1, 2 * part * width : (2 * part + 1) * width]
    stretch = mod[0:1, (2 * part + 1) * width : (2 * part + 2) * width]
    offset_drift = mod[1:2, 2 * part * width : (2 * part + 1) * width]
    stretch_drift = mod[1:2, (2 * part + 1) * width : (2 * part + 2) * width]
    primal = (normed * (1.0 + stretch) + offset).astype(BF16)
    moving = (drift * (1.0 + stretch) + normed * stretch_drift + offset_drift).astype(BF16)
    return primal, moving


def side(axis, phase):
    at = lax.axis_index(axis)
    after = (at & 1) == phase
    exists = jnp.where(after, at + 1 < lax.axis_size(axis), at > 0)
    return after, exists


def couples(count, phase):
    return [
        edge for i in range(phase, count - 1, 2) for edge in ((i, i + 1), (i + 1, i))
    ]


def exchanged(value, axis, phase):
    return lax.ppermute(value, axis, couples(lax.axis_size(axis), phase))


def partner(count, step, back=False):
    if count & (count - 1) == 0:
        return [(i, i ^ step) for i in range(count)]
    return [(i, (i - step if back else i + step) % count) for i in range(count)]


def gathered(value, axis):
    count = lax.axis_size(axis)
    return [value] + [
        lax.ppermute(value, axis, partner(count, step)) for step in range(1, count)
    ]


def row_gathered(value, axis):
    count = lax.axis_size(axis)
    if count < 4 or count & (count - 1):
        return gathered(value, axis)
    part = jnp.concatenate(
        [value] + [lax.ppermute(value, axis, partner(count, step)) for step in range(2, count, 2)],
        0,
    )
    return [part, lax.ppermute(part, axis, partner(count, 1))]


def returned(pieces, axis):
    count = lax.axis_size(axis)
    return [
        lax.ppermute(piece, axis, partner(count, step, True))
        for step, piece in zip(range(1, count), pieces)
    ]


def lanes_of(head):
    lane = lax.broadcasted_iota(jnp.int32, (1, LANES), 1)
    first = lane < head
    return (
        first,
        first.astype(F32).astype(BF16),
        (lane >= head).astype(F32).astype(BF16),
    )


def filled(array):
    short = -array.shape[0] % LANES
    if not short:
        return array
    return jnp.concatenate([array, jnp.zeros((short, array.shape[1]), array.dtype)], 0)


def attend(items, mask, head):
    count, keys = mask.shape
    first, mine, other = lanes_of(head)
    products = []
    for query, query_drift, key, key_drift, *_ in items:
        left = jnp.concatenate([query, query_drift], 1)
        left = jnp.concatenate(
            [left * jnp.concatenate([m, m], 1) for m in (mine, other)], 0
        )
        right = jnp.concatenate(
            [
                jnp.concatenate([key, jnp.zeros_like(key)], 1),
                jnp.concatenate([key_drift, key], 1),
            ],
            0,
        )
        products.append(dot_nt(left, right))
    rows = []
    for product, item in zip(products, items):
        for place, factor in enumerate(item[6]):
            block = product[place * count : (place + 1) * count]
            weight = jnp.exp2(block[:, :keys] * (factor * LOG2E)) * mask
            tilt = weight * (block[:, keys:] * factor)
            rows.append(jnp.concatenate([weight.astype(BF16), tilt.astype(BF16)], 0))
    results = []
    for i, item in enumerate(items):
        value, value_drift = item[4], item[5]
        own = dot(rows[2 * i], jnp.concatenate([value * mine + other, value_drift * mine], 1))
        next_own = dot(
            rows[2 * i + 1], jnp.concatenate([value * other + mine, value_drift * other], 1)
        )
        top, top_next = own[:count, :LANES], next_own[:count, :LANES]
        low, low_next = own[count:, :LANES], next_own[count:, :LANES]
        results.append(
            (
                jnp.where(first, top, top_next),
                jnp.where(first, own[:count, LANES:] + low, next_own[:count, LANES:] + low_next),
                jnp.where(first, top_next, top),
                jnp.where(first, low_next, low),
            )
        )
    return results


def near(key_row, key_column, columns, count):
    place = lax.broadcasted_iota(jnp.int32, (count, 1), 0)
    shift = columns.bit_length() - 1
    row = lax.shift_right_logical(place, shift)
    column = place & (columns - 1)
    close = (jnp.abs(row - key_row) <= RADIUS) & (jnp.abs(column - key_column) <= RADIUS)
    return jnp.where(close, 1.0, 0.0)


def one_hot(rows, place, valid):
    row = lax.broadcasted_iota(jnp.int32, (rows, place.shape[1]), 0)
    return jnp.where((row == place) & valid, 1.0, 0.0).astype(BF16)


def log2(number):
    return number.bit_length() - 1


def by_radius(number):
    return lax.shift_right_logical(number * (128 // RADIUS + 1), 7)


def pack_kernel(key, value, key_drift, value_drift, query, query_drift, scale, *refs):
    y0, y1, z0, z1, sems = *refs[:4], refs[-1]
    near = refs[4:11]
    far = (key, value, key_drift, value_drift, query, query_drift, scale)
    copies = [
        pltpu.make_async_copy(source, target, sems.at[i])
        for i, (source, target) in enumerate(zip(far, near))
    ]
    for copy in copies:
        copy.start()
    rows, columns, width = key.shape
    count = rows * columns
    strip = RADIUS * columns
    band = z0.shape[0] // 4
    place = lax.broadcasted_iota(jnp.int32, (1, count), 1)
    row = lax.shift_right_logical(place, log2(columns))
    picks, starts = [], []
    for phase in range(2):
        right, _ = side("tx", phase)
        column = (place & (columns - 1)) - jnp.where(right, columns - RADIUS, 0)
        valid = (column >= 0) & (column < RADIUS)
        picks.append(one_hot(band, row * RADIUS + column, valid))
        down, _ = side("ty", phase)
        starts.append(jnp.where(down, rows - RADIUS, 0))
    for array, ref in enumerate(near[:4]):
        copies[array].wait()
        flat = ref[...].reshape(count, width)
        for start, pick, y, z in zip(starts, picks, (y0, y1), (z0, z1)):
            y[array * strip : (array + 1) * strip] = ref[pl.ds(start, RADIUS)].reshape(
                strip, width
            )
            z[array * band : (array + 1) * band] = dot(pick, flat).astype(BF16)
    for copy in copies[4:]:
        copy.wait()


def corner_kernel(rows, z0, z1, c0, c1):
    half = z0.shape[0]
    side_tokens = half // 4
    square = RADIUS * RADIUS
    place = lax.broadcasted_iota(jnp.int32, (1, half), 1)
    array = sum(jnp.where(place >= i * side_tokens, 1, 0) for i in range(1, 4))
    for phase, c in enumerate((c0, c1)):
        down, _ = side("ty", phase)
        token = place - array * side_tokens - jnp.where(down, (rows - RADIUS) * RADIUS, 0)
        valid = (token >= 0) & (token < square)
        total = None
        for meet, z in enumerate((z0, z1)):
            at = (2 * array + meet) * square + token
            part = dot(one_hot(c.shape[0], at, valid), z[...])
            total = part if total is None else total + part
        c[...] = total.astype(BF16)


def wide_pairs(parts, width, ones):
    wide = math.gcd(width, WIDE)
    normed = head_pairs([parts(slice(at, at + wide)) for at in range(0, width, wide)], ones)
    return [
        tuple(filled(member[:, at : at + LANES]) for member in couple)
        for couple in normed
        for at in range(0, wide, LANES)
    ]


def factors_of(scale, pair, head):
    return [scale[2 * pair + i] / head for i in range(2)]


def pair_lanes(width):
    return [slice(at, at + LANES) for at in range(0, width, LANES)]


def own_kernel(head, scale, q, qd, k, kd, v, vd, qn, qdn, *sums):
    rows, columns, width = q.shape
    count = rows * columns
    ones = block_ones(math.gcd(width, WIDE), log2(head), 1.0 / head)
    place = lax.broadcasted_iota(jnp.int32, (1, count), 1)
    mask = near(
        lax.shift_right_logical(place, log2(columns)), place & (columns - 1), columns, count
    )

    def flat(ref, at):
        return ref[:, :, at].reshape(count, -1)

    def normed(values, tangent):
        return wide_pairs(
            lambda at: (flat(values, at).astype(F32), flat(tangent, at).astype(F32)), width, ones
        )

    queries, keys = normed(q, qd), normed(k, kd)
    items = []
    for pair, at in enumerate(pair_lanes(width)):
        qn[:, at], qdn[:, at] = queries[pair]
        items.append(
            (
                *queries[pair], *keys[pair], flat(v, at), flat(vd, at),
                factors_of(scale, pair, head),
            )
        )
    for at, parts in zip(pair_lanes(width), attend(items, mask, head)):
        for ref, part in zip(sums, parts):
            ref[:, at] = part


def moved(row, column, phase_down, phase_right, tile):
    rows, columns = tile
    outside = 4 * (rows + columns)
    for phase in range(2):
        down, below = side("ty", phase)
        right, beside = side("tx", phase)
        row_move = jnp.where(below, jnp.where(down, rows, -RADIUS), outside)
        column_move = jnp.where(beside, jnp.where(right, columns, -RADIUS), outside)
        row = row + jnp.where(phase_down == phase, row_move, 0)
        column = column + jnp.where(phase_right == phase, column_move, 0)
    return row, column


def beside_places(tile):
    rows, columns = tile
    side_tokens, strip = RADIUS * rows, RADIUS * columns
    place = lax.broadcasted_iota(jnp.int32, (1, LANES), 1)
    beside = place < 2 * side_tokens
    later = place >= side_tokens
    token = place - jnp.where(later, side_tokens, 0)
    side_row = by_radius(token)
    rest = place - 2 * side_tokens
    rest_row = lax.shift_right_logical(rest, log2(columns))
    row = jnp.where(beside, side_row, jnp.where(rest < strip, rest_row, 8 * sum(tile)))
    column = jnp.where(beside, token - side_row * RADIUS, rest & (columns - 1))
    right = jnp.where(beside, jnp.where(later, 1, 0), -1)
    return moved(row, column, jnp.where(beside, -1, 0), right, tile)


def last_places(tile):
    _, columns = tile
    strip, square = RADIUS * columns, RADIUS * RADIUS
    place = lax.broadcasted_iota(jnp.int32, (1, LANES), 1)
    level = place < strip
    slot = place - strip
    second = slot >= 2 * square
    token = slot - jnp.where(second, 2 * square, 0)
    later = token >= square
    token = token - jnp.where(later, square, 0)
    corner_row = by_radius(token)
    row = jnp.where(level, lax.shift_right_logical(place, log2(columns)), corner_row)
    column = jnp.where(level, place & (columns - 1), token - corner_row * RADIUS)
    row = jnp.where(slot < 4 * square, row, 8 * sum(tile))
    down = jnp.where(level, 1, jnp.where(second, 1, 0))
    return moved(row, column, down, jnp.where(level, -1, jnp.where(later, 1, 0)), tile)


def beside_kernel(head, tile, scale, qn, qdn, z0, z1, y0, *sums):
    width = qn.shape[1]
    ones = block_ones(math.gcd(width, WIDE), log2(head), 1.0 / head)
    mask = near(*beside_places(tile), tile[1], qn.shape[0])

    def part(array, at):
        pieces = []
        for ref in (z0, z1, y0):
            size = ref.shape[0] // 4
            pieces.append(ref[array * size : (array + 1) * size, at].astype(F32))
        return jnp.concatenate(pieces, 0)

    keys = wide_pairs(lambda at: (part(0, at), part(2, at)), width, ones)
    items = [
        (
            qn[:, at], qdn[:, at], *keys[pair], filled(part(1, at)).astype(BF16),
            filled(part(3, at)).astype(BF16), factors_of(scale, pair, head),
        )
        for pair, at in enumerate(pair_lanes(width))
    ]
    for at, parts in zip(pair_lanes(width), attend(items, mask, head)):
        for before, after, piece in zip(sums[:4], sums[4:], parts):
            after[:, at] = before[:, at] + piece


def last_kernel(
    head, tile, scale, qn, qdn, y1, c0, c1, a, ce, l, b, weight, out, tangent, coarse, pooled
):
    _, columns = tile
    count, width = qn.shape
    ones = block_ones(math.gcd(width, WIDE), log2(head), 1.0 / head)
    mask = near(*last_places(tile), columns, count)
    corner_rows = c0.shape[0]
    corner_keys = corner_rows // 4
    size = y1.shape[0] // 4
    place = lax.broadcasted_iota(jnp.int32, (1, corner_rows), 1)
    band = -(-2 * corner_keys // 8) * 8
    own = pooled.shape[0] // 2

    def part(array, at):
        slot = place - array * corner_keys
        valid = (slot >= 0) & (slot < corner_keys)
        corners = dot(one_hot(band, slot, valid), c0[:, at]) + dot(
            one_hot(band, slot + corner_keys, valid), c1[:, at]
        )
        strip = y1[array * size : (array + 1) * size, at].astype(F32)
        return jnp.concatenate([strip, corners], 0)

    whole = slice(0, width)
    values, value_drifts = (filled(part(array, whole)).astype(BF16) for array in (1, 3))
    key_values, key_drifts = part(0, whole), part(2, whole)
    keys = wide_pairs(lambda at: (key_values[:, at], key_drifts[:, at]), width, ones)
    items = [
        (
            qn[:, at], qdn[:, at], *keys[pair], values[:, at], value_drifts[:, at],
            factors_of(scale, pair, head),
        )
        for pair, at in enumerate(pair_lanes(width))
    ]
    place = lax.broadcasted_iota(jnp.int32, (1, count), 1)
    block = lax.shift_right_logical(place, log2(columns) + log2(MERGE)) * (columns // MERGE)
    block = block + lax.shift_right_logical(place & (columns - 1), log2(MERGE))
    pool = one_hot(own, block, block >= 0) * jnp.asarray(1 / (MERGE * MERGE), BF16)
    for at, parts in zip(pair_lanes(width), attend(items, mask, head)):
        inverse = 1.0 / pltpu.roll(l[:, at] + parts[2], head, 1)
        lean = pltpu.roll(b[:, at] + parts[3], head, 1)
        output = (a[:, at] + parts[0]) * inverse
        moving = (ce[:, at] + parts[1]) * inverse - output * (lean * inverse)
        output = output.astype(BF16)
        moving = moving.astype(BF16)
        out[:, :, at] = output.reshape(*tile, LANES)
        tangent[:, :, at] = moving.reshape(*tile, LANES)
        pooled[:own, at] = dot(pool, output)
        pooled[own:, at] = dot(pool, moving)
    coarse[...] = dot(pooled[...].astype(BF16), weight[...]).astype(BF16)


def stacked(refs):
    halves = [ref[...].astype(F32) for ref in refs]
    own = halves[0].shape[0] // 2
    return (
        jnp.concatenate([half[:own] for half in halves], 0),
        jnp.concatenate([half[own:] for half in halves], 0),
    )


def project_kernel(head, slots, mod, weight, *refs):
    tokens, (query_out, keys_out) = refs[:slots], refs[slots:]
    primal, moving = stacked(tokens)
    width = primal.shape[1]
    count = primal.shape[0]
    both = jnp.concatenate(conditioned(primal, moving, mod, 0, width), 0)
    heads = weight.shape[0] // (3 * head)
    span = heads * head
    ones = block_ones(span, head.bit_length() - 1, 1.0 / head)

    def projected(member):
        rows = [weight[(3 * h + member) * head : (3 * h + member + 1) * head] for h in range(heads)]
        result = dot_nt(both, jnp.concatenate(rows, 0))
        return result[:count], result[count:]

    query, key = head_pairs([projected(0), projected(1)], ones)
    value, value_drift = projected(2)
    query_out[...] = jnp.concatenate(query, 1)
    keys_out[...] = jnp.concatenate(
        [key[0], value.astype(BF16), key[1], value_drift.astype(BF16)], 1
    )


def coarse_kernel(head, slots, groups, scale, weight, query, *refs):
    blocks, outs = refs[:groups], refs[groups:]
    count = query.shape[0]
    span = query.shape[1] // 2
    heads = span // head

    def part(member):
        return jnp.concatenate(
            [block[:, member * span : (member + 1) * span] for block in blocks], 0
        )

    key, value, key_drift, value_drift = (part(member) for member in range(4))
    lane = lax.broadcasted_iota(jnp.int32, (1, span), 1)
    masks = [
        ((lane >= h * head) & (lane < (h + 1) * head)).astype(F32) for h in range(heads)
    ]
    plain, drifting = query[:, :span], query[:, span:]
    plain = jnp.concatenate([plain * mask.astype(BF16) for mask in masks], 0)
    drifting = jnp.concatenate([drifting * mask.astype(BF16) for mask in masks], 0)
    score = dot_nt(plain, key)
    slope = dot_nt(drifting, key) + dot_nt(plain, key_drift)
    weights, tilted = [], []
    for h in range(heads):
        rows = slice(h * count, (h + 1) * count)
        factor = scale[h] / head
        e = jnp.exp2(score[rows] * (factor * LOG2E))
        weights.append(e)
        tilted.append(e * (slope[rows] * factor))
    weights = jnp.concatenate(weights, 0).astype(BF16)
    tilted = jnp.concatenate(tilted, 0).astype(BF16)
    ones = jnp.ones((key.shape[0], span), BF16)

    def own(stack):
        return sum(
            stack[h * count : (h + 1) * count] * mask for h, mask in enumerate(masks)
        )

    inverse = 1.0 / own(dot(weights, ones))
    output = own(dot(weights, value)) * inverse
    shifted = own(dot(tilted, value) + dot(weights, value_drift))
    moving = shifted * inverse - output * (own(dot(tilted, ones)) * inverse)
    both = jnp.concatenate([output.astype(BF16), moving.astype(BF16)], 0)
    spread(dot(both, weight[...]), slots, outs)


def spread(both, slots, outs):
    count = both.shape[0] // 2
    own = count // slots
    for slot, out in enumerate(outs):
        piece = jnp.concatenate(
            [both[slot * own : (slot + 1) * own], both[count + slot * own : count + (slot + 1) * own]],
            0,
        )
        out[...] = piece.astype(out.dtype)


def update_kernel(slots, mod, coarse, *refs):
    parts, (updated, source) = refs[:slots], refs[slots:]
    total = coarse[...].astype(F32)
    for ref in parts:
        total = total + ref[...].astype(F32)
    updated[...] = total
    own, width = total.shape[0] // 2, total.shape[1]
    source[...] = jnp.concatenate(conditioned(total[:own], total[own:], mod, 1, width), 0)


def mlp_kernel(slots, up, down, *refs):
    tokens, outs = refs[:slots], refs[slots:]
    primal, moving = stacked(tokens)
    count = primal.shape[0]
    both = jnp.concatenate([primal, moving], 0).astype(BF16)
    hidden = dot(both, up[...])
    x, dx = hidden[:count], hidden[count:]
    root = math.sqrt(2.0 / math.pi)
    square = x * x
    bend = jnp.tanh(root * (x + 0.044715 * (square * x)))
    half = 0.5 * (1.0 + bend)
    rise = half + 0.5 * x * (1.0 - bend * bend) * (root * (1.0 + 3 * 0.044715 * square))
    active = jnp.concatenate([(x * half).astype(BF16), (rise * dx).astype(BF16)], 0)
    spread(dot(active, down[...]), slots, outs)


def final_kernel(slots, updated, *refs):
    parts, (out, tangent) = refs[:slots], refs[slots:]
    total = updated[...]
    for ref in parts:
        total = total + ref[...].astype(F32)
    own = total.shape[0] // 2
    out[...] = total[:own].astype(BF16).reshape(out.shape)
    tangent[...] = total[own:].astype(BF16).reshape(out.shape)


def modulation_kernel(index, weight, out):
    latest = jnp.maximum(index[0], index[1])
    earlier = jnp.minimum(index[0], index[1])
    halves = EMBED // 2
    row = lax.broadcasted_iota(jnp.int32, (EMBED, LANES), 0)
    angular = jnp.exp2((row & (halves - 1)).astype(F32) * (4.0 / halves))
    steps = jnp.where(row < halves, latest, latest - earlier).astype(F32) / STEPS
    angle = angular * steps
    cosine, sine = jnp.cos(angle), jnp.sin(angle)
    rise, fall = angular * cosine, -angular * sine
    feature = jnp.concatenate([cosine[:halves], sine[:halves], cosine[halves:], sine[halves:]], 0)
    slope = jnp.concatenate([fall[:halves], rise[:halves], fall[halves:], rise[halves:]], 0)
    for at in pair_lanes(weight.shape[1]):
        block = weight[:, at]
        out[0:1, at] = jnp.sum(feature * block, axis=0, keepdims=True)
        out[1:2, at] = jnp.sum(slope * block, axis=0, keepdims=True)


def struct(shape, dtype=BF16):
    return jax.ShapeDtypeStruct(shape, dtype)


def near_call(kernel, outs, args, smem_count=0, scratch=(), far_out=False):
    def near_spec():
        return pl.BlockSpec(memory_space=pltpu.VMEM)

    args = [
        a if i < smem_count else pltpu.with_memory_space_constraint(a, pltpu.VMEM)
        for i, a in enumerate(args)
    ]
    return pl.pallas_call(
        kernel,
        in_specs=[pl.BlockSpec(memory_space=pltpu.SMEM)] * smem_count
        + [near_spec()] * (len(args) - smem_count),
        out_specs=[pl.BlockSpec() if far_out else near_spec() for _ in outs],
        out_shape=outs if far_out else [pltpu.VMEM(o.shape, o.dtype) for o in outs],
        scratch_shapes=list(scratch),
        compiler_params=pltpu.CompilerParams(vmem_limit_bytes=16 * 1024 * 1024),
    )(*args)


def shards(
    queries,
    fine_key_rows,
    fine_value_rows,
    fine_query_tangent,
    fine_key_tangent,
    fine_value_tangent,
    fine_head_scale,
    merged_token_weight,
    time_plan_index,
    time_modulation_weight,
    coarse_projection_weight,
    coarse_head_scale,
    head_output_weight,
    up_projection_weight,
    down_projection_weight,
):
    rows, columns, width = queries.shape
    heads = fine_head_scale.shape[0]
    head = width // heads
    count = rows * columns
    tile = (rows, columns)
    strip = RADIUS * columns
    side_tokens = RADIUS * rows
    corner_rows = 8 * RADIUS * RADIUS
    blocks = (rows // MERGE, columns // MERGE)
    own = blocks[0] * blocks[1]

    near = pl.BlockSpec(memory_space=pltpu.VMEM)
    messages = [pltpu.VMEM((4 * strip, width), BF16)] * 2
    messages += [pltpu.VMEM((4 * side_tokens, width), BF16)] * 2
    y0, y1, z0, z1, *fine = pl.pallas_call(
        pack_kernel,
        in_specs=[pl.BlockSpec(memory_space=pltpu.HBM)] * 7,
        out_specs=[near] * 10 + [pl.BlockSpec(memory_space=pltpu.SMEM)],
        out_shape=messages
        + [pltpu.VMEM(queries.shape, BF16)] * 6
        + [pltpu.SMEM(fine_head_scale.shape, F32)],
        scratch_shapes=[pltpu.SemaphoreType.DMA((7,))],
        compiler_params=pltpu.CompilerParams(vmem_limit_bytes=16 * 1024 * 1024),
        name="pack",
    )(
        *(
            pltpu.with_memory_space_constraint(field, pltpu.HBM)
            for field in (
                fine_key_rows, fine_value_rows, fine_key_tangent, fine_value_tangent,
                queries, fine_query_tangent, fine_head_scale,
            )
        )
    )
    key, value, key_drift, value_drift, query, query_drift, scale = fine
    scale = pltpu.with_memory_space_constraint(scale, pltpu.SMEM)
    across_count = lax.axis_size("tx")
    y1 = exchanged(y1, "ty", 1)
    z0 = exchanged(z0, "tx", 0)
    z1 = exchanged(z1, "tx", 1)
    y0 = exchanged(y0, "ty", 0)

    flat = struct((count, width))
    sums = [struct((count, width), F32)] * 4
    qn, qdn, *own_sums = near_call(
        functools.partial(own_kernel, head),
        [flat] * 2 + sums,
        (
            scale, query, query_drift, key, key_drift, value, value_drift,
        ),
        1,
    )
    z0, z1, qn = lax.optimization_barrier((z0, z1, qn))
    corner = struct((corner_rows, width))
    c0, c1 = near_call(functools.partial(corner_kernel, rows), [corner] * 2, (z0, z1))
    c1 = exchanged(c1, "ty", 1)
    c0 = exchanged(c0, "ty", 0)
    beside_sums = near_call(
        functools.partial(beside_kernel, head, tile),
        sums,
        (scale, qn, qdn, z0, z1, y0, *own_sums),
        1,
    )
    grid_shape = struct(queries.shape)
    pooled = struct((2 * own, width))
    fine_out, fine_tangent, coarse = near_call(
        functools.partial(last_kernel, head, tile),
        [grid_shape] * 2 + [pooled],
        (
            scale, qn, qdn, y1, c0, c1, *beside_sums, merged_token_weight,
        ),
        1,
        [pltpu.VMEM((2 * own, width), F32)],
    )

    (mod,) = near_call(
        modulation_kernel,
        [struct((2, 4 * width), F32)],
        (time_plan_index, time_modulation_weight),
        1,
    )
    near_heads = coarse_head_scale.shape[0]
    span = near_heads * head
    packed = coarse_projection_weight.transpose(1, 2, 0).reshape(3 * span, width)
    slots = across_count
    tokens = gathered(coarse, "tx")
    group = slots * own
    query, keys = near_call(
        functools.partial(project_kernel, head, slots),
        [struct((group, 2 * span)), struct((group, 4 * span))],
        (mod, packed, *tokens),
    )
    key_blocks = row_gathered(keys, "ty")
    pieces = [struct((2 * own, width), F32)] + [struct((2 * own, width))] * (slots - 1)
    kept, *sent = near_call(
        functools.partial(coarse_kernel, head, slots, len(key_blocks)),
        pieces,
        (coarse_head_scale, head_output_weight.reshape(span, width), query, *key_blocks),
        1,
    )
    updated, source = near_call(
        functools.partial(update_kernel, slots),
        [struct((2 * own, width), F32), struct((2 * own, width))],
        (mod, coarse, kept, *returned(sent, "tx")),
    )
    kept, *sent = near_call(
        functools.partial(mlp_kernel, slots),
        pieces,
        (up_projection_weight, down_projection_weight, *gathered(source, "tx")),
    )
    coarse_out, coarse_tangent = near_call(
        functools.partial(final_kernel, slots),
        [struct((*blocks, width))] * 2,
        (updated, kept, *returned(sent, "tx")),
        far_out=True,
    )
    return (fine_out, fine_tangent, coarse_out, coarse_tangent)


def solution(mesh):
    return jax.shard_map(
        shards,
        mesh=mesh,
        in_specs=(
            P("ty", "tx", None),
            P("ty", "tx", None),
            P("ty", "tx", None),
            P("ty", "tx", None),
            P("ty", "tx", None),
            P("ty", "tx", None),
            P(),
            P(),
            P(),
            P(),
            P(None, "tx", None),
            P("tx"),
            P("tx", None, None),
            P(None, "tx"),
            P("tx", None),
        ),
        out_specs=(
            P("ty", "tx", None),
            P("ty", "tx", None),
            P("ty", "tx", None),
            P("ty", "tx", None),
        ),
        check_vma=False,
    )
```

```python
import functools
import math

import jax
import jax.numpy as jnp
from jax import lax
from jax.experimental import pallas as pl
from jax.experimental.pallas import tpu as pltpu
from jax.sharding import PartitionSpec as P


EMBED = 128
RADIUS = 3
MERGE = 4
STEPS = 1000
EPSILON = 1e-06
LANES = 128
WIDE = 256
LOG2E = math.log2(math.e)
F32 = jnp.float32
BF16 = jnp.bfloat16


def dot(a, b):
    return jnp.dot(a, b, preferred_element_type=F32)


def dot_nt(a, b):
    return lax.dot_general(a, b, (((1,), (1,)), ((), ())), preferred_element_type=F32)


def block_ones(width, head, value):
    row = lax.broadcasted_iota(jnp.int32, (width, width), 0)
    col = lax.broadcasted_iota(jnp.int32, (width, width), 1)
    same = lax.shift_right_logical(row, head) == lax.shift_right_logical(col, head)
    return jnp.where(same, value, 0.0).astype(BF16)


def head_means(arrays, ones):
    highs = [array.astype(BF16) for array in arrays]
    lows = [(a - h.astype(F32)).astype(BF16) for a, h in zip(arrays, highs)]
    means = dot(jnp.concatenate(highs, 0), ones) + dot(jnp.concatenate(lows, 0), ones)
    pieces, at = [], 0
    for array in arrays:
        pieces.append(means[at : at + array.shape[0]])
        at += array.shape[0]
    return pieces


def head_pairs(couples_of, ones):
    factors = [
        lax.rsqrt(mean + EPSILON)
        for mean in head_means([values * values for values, _ in couples_of], ones)
    ]
    normed = [values * factor for (values, _), factor in zip(couples_of, factors)]
    leans = head_means([n * tangent for n, (_, tangent) in zip(normed, couples_of)], ones)
    return [
        (n.astype(BF16), ((tangent - n * lean) * factor).astype(BF16))
        for n, (_, tangent), lean, factor in zip(normed, couples_of, leans, factors)
    ]


def row_pair(values, tangent):
    factor = lax.rsqrt(jnp.mean(values * values, axis=-1, keepdims=True) + EPSILON)
    normed = values * factor
    drift = (tangent - normed * jnp.mean(normed * tangent, axis=-1, keepdims=True)) * factor
    return normed, drift


def conditioned(values, tangent, mod, part, width):
    normed, drift = row_pair(values, tangent)
    offset = mod[0:1, 2 * part * width : (2 * part + 1) * width]
    stretch = mod[0:1, (2 * part + 1) * width : (2 * part + 2) * width]
    offset_drift = mod[1:2, 2 * part * width : (2 * part + 1) * width]
    stretch_drift = mod[1:2, (2 * part + 1) * width : (2 * part + 2) * width]
    primal = (normed * (1.0 + stretch) + offset).astype(BF16)
    moving = (drift * (1.0 + stretch) + normed * stretch_drift + offset_drift).astype(BF16)
    return primal, moving


def side(axis, phase):
    at = lax.axis_index(axis)
    after = (at & 1) == phase
    exists = jnp.where(after, at + 1 < lax.axis_size(axis), at > 0)
    return after, exists


def couples(count, phase):
    return [
        edge for i in range(phase, count - 1, 2) for edge in ((i, i + 1), (i + 1, i))
    ]


def exchanged(value, axis, phase):
    return lax.ppermute(value, axis, couples(lax.axis_size(axis), phase))


def partner(count, step, back=False):
    if count & (count - 1) == 0:
        return [(i, i ^ step) for i in range(count)]
    return [(i, (i - step if back else i + step) % count) for i in range(count)]


def gathered(value, axis):
    count = lax.axis_size(axis)
    return [value] + [
        lax.ppermute(value, axis, partner(count, step)) for step in range(count - 1, 0, -1)
    ]


def row_gathered(value, axis):
    count = lax.axis_size(axis)
    if count < 4 or count & (count - 1):
        return gathered(value, axis)
    part = jnp.concatenate(
        [value] + [lax.ppermute(value, axis, partner(count, step)) for step in range(count - 2, 0, -2)],
        0,
    )
    return [part, lax.ppermute(part, axis, partner(count, 1))]


def returned(pieces, axis):
    count = lax.axis_size(axis)
    return [
        lax.ppermute(piece, axis, partner(count, step, True))
        for step, piece in zip(range(count - 1, 0, -1), pieces)
    ]


def lanes_of(head):
    lane = lax.broadcasted_iota(jnp.int32, (1, LANES), 1)
    first = lane < head
    return (
        first,
        first.astype(F32).astype(BF16),
        (lane >= head).astype(F32).astype(BF16),
    )


def filled(array):
    short = -array.shape[0] % LANES
    if not short:
        return array
    return jnp.concatenate([array, jnp.zeros((short, array.shape[1]), array.dtype)], 0)


def attend(items, mask, head):
    count, keys = mask.shape
    first, mine, other = lanes_of(head)
    products = []
    for query, query_drift, key, key_drift, *_ in items:
        left = jnp.concatenate([query, query_drift], 1)
        left = jnp.concatenate(
            [left * jnp.concatenate([m, m], 1) for m in (mine, other)], 0
        )
        right = jnp.concatenate(
            [
                jnp.concatenate([key, jnp.zeros_like(key)], 1),
                jnp.concatenate([key_drift, key], 1),
            ],
            0,
        )
        products.append(dot_nt(left, right))
    rows = []
    for product, item in zip(products, items):
        for place, factor in enumerate(item[6]):
            block = product[place * count : (place + 1) * count]
            weight = jnp.exp2(block[:, :keys] * (factor * LOG2E)) * mask
            tilt = weight * (block[:, keys:] * factor)
            rows.append(jnp.concatenate([weight.astype(BF16), tilt.astype(BF16)], 0))
    results = []
    for i, item in enumerate(items):
        value, value_drift = item[4], item[5]
        own = dot(rows[2 * i], jnp.concatenate([value * mine + other, value_drift * mine], 1))
        next_own = dot(
            rows[2 * i + 1], jnp.concatenate([value * other + mine, value_drift * other], 1)
        )
        top, top_next = own[:count, :LANES], next_own[:count, :LANES]
        low, low_next = own[count:, :LANES], next_own[count:, :LANES]
        results.append(
            (
                jnp.where(first, top, top_next),
                jnp.where(first, own[:count, LANES:] + low, next_own[:count, LANES:] + low_next),
                jnp.where(first, top_next, top),
                jnp.where(first, low_next, low),
            )
        )
    return results


def near(key_row, key_column, columns, count):
    place = lax.broadcasted_iota(jnp.int32, (count, 1), 0)
    shift = columns.bit_length() - 1
    row = lax.shift_right_logical(place, shift)
    column = place & (columns - 1)
    close = (jnp.abs(row - key_row) <= RADIUS) & (jnp.abs(column - key_column) <= RADIUS)
    return jnp.where(close, 1.0, 0.0)


def one_hot(rows, place, valid):
    row = lax.broadcasted_iota(jnp.int32, (rows, place.shape[1]), 0)
    return jnp.where((row == place) & valid, 1.0, 0.0).astype(BF16)


def log2(number):
    return number.bit_length() - 1


def by_radius(number):
    return lax.shift_right_logical(number * (128 // RADIUS + 1), 7)


def pack_kernel(key, value, key_drift, value_drift, query, query_drift, scale, *refs):
    y0, y1, z0, z1, sems = *refs[:4], refs[-1]
    near = refs[4:11]
    far = (key, value, key_drift, value_drift, query, query_drift, scale)
    copies = [
        pltpu.make_async_copy(source, target, sems.at[i])
        for i, (source, target) in enumerate(zip(far, near))
    ]
    for copy in copies:
        copy.start()
    rows, columns, width = key.shape
    count = rows * columns
    strip = RADIUS * columns
    band = z0.shape[0] // 4
    place = lax.broadcasted_iota(jnp.int32, (1, count), 1)
    row = lax.shift_right_logical(place, log2(columns))
    picks, starts = [], []
    for phase in range(2):
        right, _ = side("tx", phase)
        column = (place & (columns - 1)) - jnp.where(right, columns - RADIUS, 0)
        valid = (column >= 0) & (column < RADIUS)
        picks.append(one_hot(band, row * RADIUS + column, valid))
        down, _ = side("ty", phase)
        starts.append(jnp.where(down, rows - RADIUS, 0))
    for array, ref in enumerate(near[:4]):
        copies[array].wait()
        flat = ref[...].reshape(count, width)
        for start, pick, y, z in zip(starts, picks, (y0, y1), (z0, z1)):
            y[array * strip : (array + 1) * strip] = ref[pl.ds(start, RADIUS)].reshape(
                strip, width
            )
            z[array * band : (array + 1) * band] = dot(pick, flat).astype(BF16)
    for copy in copies[4:]:
        copy.wait()


def corner_kernel(rows, z0, z1, c0, c1):
    half = z0.shape[0]
    side_tokens = half // 4
    square = RADIUS * RADIUS
    place = lax.broadcasted_iota(jnp.int32, (1, half), 1)
    array = sum(jnp.where(place >= i * side_tokens, 1, 0) for i in range(1, 4))
    for phase, c in enumerate((c0, c1)):
        down, _ = side("ty", phase)
        token = place - array * side_tokens - jnp.where(down, (rows - RADIUS) * RADIUS, 0)
        valid = (token >= 0) & (token < square)
        total = None
        for meet, z in enumerate((z0, z1)):
            at = (2 * array + meet) * square + token
            part = dot(one_hot(c.shape[0], at, valid), z[...])
            total = part if total is None else total + part
        c[...] = total.astype(BF16)


def wide_pairs(parts, width, ones):
    wide = math.gcd(width, WIDE)
    normed = head_pairs([parts(slice(at, at + wide)) for at in range(0, width, wide)], ones)
    return [
        tuple(filled(member[:, at : at + LANES]) for member in couple)
        for couple in normed
        for at in range(0, wide, LANES)
    ]


def factors_of(scale, pair, head):
    return [scale[2 * pair + i] / head for i in range(2)]


def pair_lanes(width):
    return [slice(at, at + LANES) for at in range(0, width, LANES)]


def own_kernel(head, scale, q, qd, k, kd, v, vd, qn, qdn, *sums):
    rows, columns, width = q.shape
    count = rows * columns
    ones = block_ones(math.gcd(width, WIDE), log2(head), 1.0 / head)
    place = lax.broadcasted_iota(jnp.int32, (1, count), 1)
    mask = near(
        lax.shift_right_logical(place, log2(columns)), place & (columns - 1), columns, count
    )

    def flat(ref, at):
        return ref[:, :, at].reshape(count, -1)

    def normed(values, tangent):
        return wide_pairs(
            lambda at: (flat(values, at).astype(F32), flat(tangent, at).astype(F32)), width, ones
        )

    queries, keys = normed(q, qd), normed(k, kd)
    items = []
    for pair, at in enumerate(pair_lanes(width)):
        qn[:, at], qdn[:, at] = queries[pair]
        items.append(
            (
                *queries[pair], *keys[pair], flat(v, at), flat(vd, at),
                factors_of(scale, pair, head),
            )
        )
    for at, parts in zip(pair_lanes(width), attend(items, mask, head)):
        for ref, part in zip(sums, parts):
            ref[:, at] = part


def moved(row, column, phase_down, phase_right, tile):
    rows, columns = tile
    outside = 4 * (rows + columns)
    for phase in range(2):
        down, below = side("ty", phase)
        right, beside = side("tx", phase)
        row_move = jnp.where(below, jnp.where(down, rows, -RADIUS), outside)
        column_move = jnp.where(beside, jnp.where(right, columns, -RADIUS), outside)
        row = row + jnp.where(phase_down == phase, row_move, 0)
        column = column + jnp.where(phase_right == phase, column_move, 0)
    return row, column


def beside_places(tile):
    rows, columns = tile
    side_tokens, strip = RADIUS * rows, RADIUS * columns
    place = lax.broadcasted_iota(jnp.int32, (1, LANES), 1)
    beside = place < 2 * side_tokens
    later = place >= side_tokens
    token = place - jnp.where(later, side_tokens, 0)
    side_row = by_radius(token)
    rest = place - 2 * side_tokens
    rest_row = lax.shift_right_logical(rest, log2(columns))
    row = jnp.where(beside, side_row, jnp.where(rest < strip, rest_row, 8 * sum(tile)))
    column = jnp.where(beside, token - side_row * RADIUS, rest & (columns - 1))
    right = jnp.where(beside, jnp.where(later, 1, 0), -1)
    return moved(row, column, jnp.where(beside, -1, 0), right, tile)


def last_places(tile):
    _, columns = tile
    strip, square = RADIUS * columns, RADIUS * RADIUS
    place = lax.broadcasted_iota(jnp.int32, (1, LANES), 1)
    level = place < strip
    slot = place - strip
    second = slot >= 2 * square
    token = slot - jnp.where(second, 2 * square, 0)
    later = token >= square
    token = token - jnp.where(later, square, 0)
    corner_row = by_radius(token)
    row = jnp.where(level, lax.shift_right_logical(place, log2(columns)), corner_row)
    column = jnp.where(level, place & (columns - 1), token - corner_row * RADIUS)
    row = jnp.where(slot < 4 * square, row, 8 * sum(tile))
    down = jnp.where(level, 1, jnp.where(second, 1, 0))
    return moved(row, column, down, jnp.where(level, -1, jnp.where(later, 1, 0)), tile)


def beside_kernel(head, tile, scale, qn, qdn, z0, z1, y0, *sums):
    width = qn.shape[1]
    ones = block_ones(math.gcd(width, WIDE), log2(head), 1.0 / head)
    mask = near(*beside_places(tile), tile[1], qn.shape[0])

    def part(array, at):
        pieces = []
        for ref in (z0, z1, y0):
            size = ref.shape[0] // 4
            pieces.append(ref[array * size : (array + 1) * size, at].astype(F32))
        return jnp.concatenate(pieces, 0)

    keys = wide_pairs(lambda at: (part(0, at), part(2, at)), width, ones)
    items = [
        (
            qn[:, at], qdn[:, at], *keys[pair], filled(part(1, at)).astype(BF16),
            filled(part(3, at)).astype(BF16), factors_of(scale, pair, head),
        )
        for pair, at in enumerate(pair_lanes(width))
    ]
    for at, parts in zip(pair_lanes(width), attend(items, mask, head)):
        for before, after, piece in zip(sums[:4], sums[4:], parts):
            after[:, at] = before[:, at] + piece


def last_kernel(
    head, tile, scale, qn, qdn, y1, c0, c1, a, ce, l, b, weight, out, tangent, coarse, pooled
):
    _, columns = tile
    count, width = qn.shape
    ones = block_ones(math.gcd(width, WIDE), log2(head), 1.0 / head)
    mask = near(*last_places(tile), columns, count)
    corner_rows = c0.shape[0]
    corner_keys = corner_rows // 4
    size = y1.shape[0] // 4
    place = lax.broadcasted_iota(jnp.int32, (1, corner_rows), 1)
    band = -(-2 * corner_keys // 8) * 8
    own = pooled.shape[0] // 2

    def part(array, at):
        slot = place - array * corner_keys
        valid = (slot >= 0) & (slot < corner_keys)
        corners = dot(one_hot(band, slot, valid), c0[:, at]) + dot(
            one_hot(band, slot + corner_keys, valid), c1[:, at]
        )
        strip = y1[array * size : (array + 1) * size, at].astype(F32)
        return jnp.concatenate([strip, corners], 0)

    whole = slice(0, width)
    values, value_drifts = (filled(part(array, whole)).astype(BF16) for array in (1, 3))
    key_values, key_drifts = part(0, whole), part(2, whole)
    keys = wide_pairs(lambda at: (key_values[:, at], key_drifts[:, at]), width, ones)
    items = [
        (
            qn[:, at], qdn[:, at], *keys[pair], values[:, at], value_drifts[:, at],
            factors_of(scale, pair, head),
        )
        for pair, at in enumerate(pair_lanes(width))
    ]
    place = lax.broadcasted_iota(jnp.int32, (1, count), 1)
    block = lax.shift_right_logical(place, log2(columns) + log2(MERGE)) * (columns // MERGE)
    block = block + lax.shift_right_logical(place & (columns - 1), log2(MERGE))
    pool = one_hot(own, block, block >= 0) * jnp.asarray(1 / (MERGE * MERGE), BF16)
    for at, parts in zip(pair_lanes(width), attend(items, mask, head)):
        inverse = 1.0 / pltpu.roll(l[:, at] + parts[2], head, 1)
        lean = pltpu.roll(b[:, at] + parts[3], head, 1)
        output = (a[:, at] + parts[0]) * inverse
        moving = (ce[:, at] + parts[1]) * inverse - output * (lean * inverse)
        output = output.astype(BF16)
        moving = moving.astype(BF16)
        out[:, :, at] = output.reshape(*tile, LANES)
        tangent[:, :, at] = moving.reshape(*tile, LANES)
        pooled[:own, at] = dot(pool, output)
        pooled[own:, at] = dot(pool, moving)
    coarse[...] = dot(pooled[...].astype(BF16), weight[...]).astype(BF16)


def stacked(refs):
    halves = [ref[...].astype(F32) for ref in refs]
    own = halves[0].shape[0] // 2
    return (
        jnp.concatenate([half[:own] for half in halves], 0),
        jnp.concatenate([half[own:] for half in halves], 0),
    )


def project_kernel(head, slots, mod, weight, *refs):
    tokens, (query_out, keys_out) = refs[:slots], refs[slots:]
    primal, moving = stacked(tokens)
    width = primal.shape[1]
    count = primal.shape[0]
    both = jnp.concatenate(conditioned(primal, moving, mod, 0, width), 0)
    heads = weight.shape[0] // (3 * head)
    span = heads * head
    ones = block_ones(span, head.bit_length() - 1, 1.0 / head)

    def projected(member):
        rows = [weight[(3 * h + member) * head : (3 * h + member + 1) * head] for h in range(heads)]
        result = dot_nt(both, jnp.concatenate(rows, 0))
        return result[:count], result[count:]

    query, key = head_pairs([projected(0), projected(1)], ones)
    value, value_drift = projected(2)
    query_out[...] = jnp.concatenate(query, 1)
    keys_out[...] = jnp.concatenate(
        [key[0], value.astype(BF16), key[1], value_drift.astype(BF16)], 1
    )


def coarse_kernel(head, slots, groups, scale, weight, query, *refs):
    blocks, outs = refs[:groups], refs[groups:]
    count = query.shape[0]
    span = query.shape[1] // 2
    heads = span // head

    def part(member):
        return jnp.concatenate(
            [block[:, member * span : (member + 1) * span] for block in blocks], 0
        )

    key, value, key_drift, value_drift = (part(member) for member in range(4))
    lane = lax.broadcasted_iota(jnp.int32, (1, span), 1)
    masks = [
        ((lane >= h * head) & (lane < (h + 1) * head)).astype(F32) for h in range(heads)
    ]
    plain, drifting = query[:, :span], query[:, span:]
    plain = jnp.concatenate([plain * mask.astype(BF16) for mask in masks], 0)
    drifting = jnp.concatenate([drifting * mask.astype(BF16) for mask in masks], 0)
    score = dot_nt(plain, key)
    slope = dot_nt(drifting, key) + dot_nt(plain, key_drift)
    weights, tilted = [], []
    for h in range(heads):
        rows = slice(h * count, (h + 1) * count)
        factor = scale[h] / head
        e = jnp.exp2(score[rows] * (factor * LOG2E))
        weights.append(e)
        tilted.append(e * (slope[rows] * factor))
    weights = jnp.concatenate(weights, 0).astype(BF16)
    tilted = jnp.concatenate(tilted, 0).astype(BF16)
    ones = jnp.ones((key.shape[0], span), BF16)

    def own(stack):
        return sum(
            stack[h * count : (h + 1) * count] * mask for h, mask in enumerate(masks)
        )

    inverse = 1.0 / own(dot(weights, ones))
    output = own(dot(weights, value)) * inverse
    shifted = own(dot(tilted, value) + dot(weights, value_drift))
    moving = shifted * inverse - output * (own(dot(tilted, ones)) * inverse)
    both = jnp.concatenate([output.astype(BF16), moving.astype(BF16)], 0)
    spread(dot(both, weight[...]), slots, outs)


def spread(both, slots, outs):
    count = both.shape[0] // 2
    own = count // slots
    for slot, out in enumerate(outs):
        piece = jnp.concatenate(
            [both[slot * own : (slot + 1) * own], both[count + slot * own : count + (slot + 1) * own]],
            0,
        )
        out[...] = piece.astype(out.dtype)


def update_kernel(slots, mod, coarse, *refs):
    parts, (updated, source) = refs[:slots], refs[slots:]
    total = coarse[...].astype(F32)
    for ref in parts:
        total = total + ref[...].astype(F32)
    updated[...] = total
    own, width = total.shape[0] // 2, total.shape[1]
    source[...] = jnp.concatenate(conditioned(total[:own], total[own:], mod, 1, width), 0)


def mlp_kernel(slots, up, down, *refs):
    tokens, outs = refs[:slots], refs[slots:]
    primal, moving = stacked(tokens)
    count = primal.shape[0]
    both = jnp.concatenate([primal, moving], 0).astype(BF16)
    hidden = dot(both, up[...])
    x, dx = hidden[:count], hidden[count:]
    root = math.sqrt(2.0 / math.pi)
    square = x * x
    bend = jnp.tanh(root * (x + 0.044715 * (square * x)))
    half = 0.5 * (1.0 + bend)
    rise = half + 0.5 * x * (1.0 - bend * bend) * (root * (1.0 + 3 * 0.044715 * square))
    active = jnp.concatenate([(x * half).astype(BF16), (rise * dx).astype(BF16)], 0)
    spread(dot(active, down[...]), slots, outs)


def final_kernel(slots, updated, *refs):
    parts, (out, tangent) = refs[:slots], refs[slots:]
    total = updated[...]
    for ref in parts:
        total = total + ref[...].astype(F32)
    own = total.shape[0] // 2
    out[...] = total[:own].astype(BF16).reshape(out.shape)
    tangent[...] = total[own:].astype(BF16).reshape(out.shape)


def modulation_kernel(index, weight, out):
    latest = jnp.maximum(index[0], index[1])
    earlier = jnp.minimum(index[0], index[1])
    halves = EMBED // 2
    row = lax.broadcasted_iota(jnp.int32, (EMBED, LANES), 0)
    angular = jnp.exp2((row & (halves - 1)).astype(F32) * (4.0 / halves))
    steps = jnp.where(row < halves, latest, latest - earlier).astype(F32) / STEPS
    angle = angular * steps
    cosine, sine = jnp.cos(angle), jnp.sin(angle)
    rise, fall = angular * cosine, -angular * sine
    feature = jnp.concatenate([cosine[:halves], sine[:halves], cosine[halves:], sine[halves:]], 0)
    slope = jnp.concatenate([fall[:halves], rise[:halves], fall[halves:], rise[halves:]], 0)
    for at in pair_lanes(weight.shape[1]):
        block = weight[:, at]
        out[0:1, at] = jnp.sum(feature * block, axis=0, keepdims=True)
        out[1:2, at] = jnp.sum(slope * block, axis=0, keepdims=True)


def struct(shape, dtype=BF16):
    return jax.ShapeDtypeStruct(shape, dtype)


def near_call(kernel, outs, args, smem_count=0, scratch=(), far_out=False):
    def near_spec():
        return pl.BlockSpec(memory_space=pltpu.VMEM)

    args = [
        a if i < smem_count else pltpu.with_memory_space_constraint(a, pltpu.VMEM)
        for i, a in enumerate(args)
    ]
    return pl.pallas_call(
        kernel,
        in_specs=[pl.BlockSpec(memory_space=pltpu.SMEM)] * smem_count
        + [near_spec()] * (len(args) - smem_count),
        out_specs=[pl.BlockSpec() if far_out else near_spec() for _ in outs],
        out_shape=outs if far_out else [pltpu.VMEM(o.shape, o.dtype) for o in outs],
        scratch_shapes=list(scratch),
        compiler_params=pltpu.CompilerParams(vmem_limit_bytes=16 * 1024 * 1024),
    )(*args)


def shards(
    queries,
    fine_key_rows,
    fine_value_rows,
    fine_query_tangent,
    fine_key_tangent,
    fine_value_tangent,
    fine_head_scale,
    merged_token_weight,
    time_plan_index,
    time_modulation_weight,
    coarse_projection_weight,
    coarse_head_scale,
    head_output_weight,
    up_projection_weight,
    down_projection_weight,
):
    rows, columns, width = queries.shape
    heads = fine_head_scale.shape[0]
    head = width // heads
    count = rows * columns
    tile = (rows, columns)
    strip = RADIUS * columns
    side_tokens = RADIUS * rows
    corner_rows = 8 * RADIUS * RADIUS
    blocks = (rows // MERGE, columns // MERGE)
    own = blocks[0] * blocks[1]

    near = pl.BlockSpec(memory_space=pltpu.VMEM)
    messages = [pltpu.VMEM((4 * strip, width), BF16)] * 2
    messages += [pltpu.VMEM((4 * side_tokens, width), BF16)] * 2
    y0, y1, z0, z1, *fine = pl.pallas_call(
        pack_kernel,
        in_specs=[pl.BlockSpec(memory_space=pltpu.HBM)] * 7,
        out_specs=[near] * 10 + [pl.BlockSpec(memory_space=pltpu.SMEM)],
        out_shape=messages
        + [pltpu.VMEM(queries.shape, BF16)] * 6
        + [pltpu.SMEM(fine_head_scale.shape, F32)],
        scratch_shapes=[pltpu.SemaphoreType.DMA((7,))],
        compiler_params=pltpu.CompilerParams(vmem_limit_bytes=16 * 1024 * 1024),
        name="pack",
    )(
        *(
            pltpu.with_memory_space_constraint(field, pltpu.HBM)
            for field in (
                fine_key_rows, fine_value_rows, fine_key_tangent, fine_value_tangent,
                queries, fine_query_tangent, fine_head_scale,
            )
        )
    )
    key, value, key_drift, value_drift, query, query_drift, scale = fine
    scale = pltpu.with_memory_space_constraint(scale, pltpu.SMEM)
    across_count = lax.axis_size("tx")
    y1 = exchanged(y1, "ty", 1)
    z0 = exchanged(z0, "tx", 0)
    z1 = exchanged(z1, "tx", 1)
    y0 = exchanged(y0, "ty", 0)

    flat = struct((count, width))
    sums = [struct((count, width), F32)] * 4
    qn, qdn, *own_sums = near_call(
        functools.partial(own_kernel, head),
        [flat] * 2 + sums,
        (
            scale, query, query_drift, key, key_drift, value, value_drift,
        ),
        1,
    )
    z0, z1, qn = lax.optimization_barrier((z0, z1, qn))
    corner = struct((corner_rows, width))
    c0, c1 = near_call(functools.partial(corner_kernel, rows), [corner] * 2, (z0, z1))
    c1 = exchanged(c1, "ty", 1)
    c0 = exchanged(c0, "ty", 0)
    beside_sums = near_call(
        functools.partial(beside_kernel, head, tile),
        sums,
        (scale, qn, qdn, z0, z1, y0, *own_sums),
        1,
    )
    grid_shape = struct(queries.shape)
    pooled = struct((2 * own, width))
    fine_out, fine_tangent, coarse = near_call(
        functools.partial(last_kernel, head, tile),
        [grid_shape] * 2 + [pooled],
        (
            scale, qn, qdn, y1, c0, c1, *beside_sums, merged_token_weight,
        ),
        1,
        [pltpu.VMEM((2 * own, width), F32)],
    )

    (mod,) = near_call(
        modulation_kernel,
        [struct((2, 4 * width), F32)],
        (time_plan_index, time_modulation_weight),
        1,
    )
    near_heads = coarse_head_scale.shape[0]
    span = near_heads * head
    packed = coarse_projection_weight.transpose(1, 2, 0).reshape(3 * span, width)
    slots = across_count
    tokens = gathered(coarse, "tx")
    group = slots * own
    query, keys = near_call(
        functools.partial(project_kernel, head, slots),
        [struct((group, 2 * span)), struct((group, 4 * span))],
        (mod, packed, *tokens),
    )
    key_blocks = row_gathered(keys, "ty")
    pieces = [struct((2 * own, width), F32)] + [struct((2 * own, width))] * (slots - 1)
    kept, *sent = near_call(
        functools.partial(coarse_kernel, head, slots, len(key_blocks)),
        pieces,
        (coarse_head_scale, head_output_weight.reshape(span, width), query, *key_blocks),
        1,
    )
    updated, source = near_call(
        functools.partial(update_kernel, slots),
        [struct((2 * own, width), F32), struct((2 * own, width))],
        (mod, coarse, kept, *returned(sent, "tx")),
    )
    kept, *sent = near_call(
        functools.partial(mlp_kernel, slots),
        pieces,
        (up_projection_weight, down_projection_weight, *gathered(source, "tx")),
    )
    coarse_out, coarse_tangent = near_call(
        functools.partial(final_kernel, slots),
        [struct((*blocks, width))] * 2,
        (updated, kept, *returned(sent, "tx")),
        far_out=True,
    )
    return (fine_out, fine_tangent, coarse_out, coarse_tangent)


def solution(mesh):
    return jax.shard_map(
        shards,
        mesh=mesh,
        in_specs=(
            P("ty", "tx", None),
            P("ty", "tx", None),
            P("ty", "tx", None),
            P("ty", "tx", None),
            P("ty", "tx", None),
            P("ty", "tx", None),
            P(),
            P(),
            P(),
            P(),
            P(None, "tx", None),
            P("tx"),
            P("tx", None, None),
            P(None, "tx"),
            P("tx", None),
        ),
        out_specs=(
            P("ty", "tx", None),
            P("ty", "tx", None),
            P("ty", "tx", None),
            P("ty", "tx", None),
        ),
        check_vma=False,
    )
```
